256 devices in a mesh: grp: 4 (over x), ty: 4 (over z_lo), tx: 16 (over z_hi, y, core).
Axes of the slice: x: 4, y: 4, z: 8 (z_hi: 2, z_lo: 4; z = z_hi * 4 + z_lo), core: 2. Of those that a mesh axis runs over, the one named last changes fastest.
Arguments:
- tracers: float32 [16, 8, 512, 2048], P(None, 'grp', 'ty', 'tx'), may hold values from -1.5 to 3, as said below
- east_velocity: float32 [8, 512, 2048], P('grp', 'ty', 'tx'), may hold values from -0.6 to 0.6
- north_velocity: float32 [8, 512, 2048], P('grp', 'ty', 'tx'), may hold values from -0.6 to 0.6
- surface: float32 [512, 2048], P('ty', 'tx'), may hold values from -1.5 to 1.5
- depth: float32 [512, 2048], P('ty', 'tx'), may hold values from 1 to 3
- wet_mask: int32 [512, 2048], P('ty', 'tx'), may hold values 0 or 1
- river_cells: int32 [256], P(('ty', 'tx')), may hold values from 0 to 16383
- river_loads: float32 [256, 16], P(('ty', 'tx')), may hold values from 0.2 to 2
- kinetics: float32 [16, 16], replicated, may hold values from -0.3 to 0.24, as said below
Outputs:
- new_tracers: float32 [16, 8, 512, 2048], P(None, 'grp', 'ty', 'tx')
- new_east: float32 [8, 512, 2048], P('grp', 'ty', 'tx')
- new_north: float32 [8, 512, 2048], P('grp', 'ty', 'tx')
- new_surface: float32 [512, 2048], P('ty', 'tx')
The draws below stay inside these ranges and needn't reach their ends.
Inputs may be any that keep to these rules, and one draw needn't show every extreme that they name: `tracers`: tracer 0 lies in -1.5 to 1.5, tracer 1 in -1 to 1, the others in 0.1 to 3. `kinetics`: diagonal entries lie in -0.3 to -0.05. `river_cells`: entry r is row * 128 + column of a cell in the tile of the device that holds entry r.
All inputs are finite; a program needn't handle non-finite values. No bound on the sum of `wet_mask` on one device may be relied on, other than what follows from the above.
Results may differ from the reference program's by a relative error of at most 0.000096.
Values sent between devices are 32-bit elements; how exact they have to be, the bound alone decides.
A program may use at most 64 MiB of HBM per device.

```python
import math
import jax
import jax.numpy as jnp
from jax import lax

NTR = 16
CY = 128
CX = 128
RIV_DEV = 4
NY = 512
NX = 2048
LEV = 8
RIVERS = 256
N_TX = 16


def draw_tracers(key, part):
    keys = jax.random.split(jax.random.fold_in(key, 11), 3)
    salinity = jax.random.uniform(keys[0], (1, LEV, NY, NX), jnp.float32, -1.5, 1.5)
    heat = jax.random.uniform(keys[1], (1, LEV, NY, NX), jnp.float32, -1.0, 1.0)
    others = jnp.exp(jax.random.uniform(keys[2], (NTR - 2, LEV, NY, NX), jnp.float32, math.log(0.1), math.log(3.0)))
    return jnp.concatenate([salinity, heat, others], 0)


def draw_kinetics(key, part):
    keys = jax.random.split(jax.random.fold_in(key, 23), 2)
    coupling = jax.random.truncated_normal(keys[0], -4.0, 4.0, (NTR, NTR), jnp.float32) * 0.06
    rates = jnp.exp(jax.random.uniform(keys[1], (NTR,), jnp.float32, math.log(0.05), math.log(0.3)))
    identity = jnp.eye(NTR, dtype=jnp.float32)
    return coupling * (1.0 - identity) - identity * rates[None, :]


def plant(drawn, stream_key, smallest, largest):
    longest = drawn.shape.index(max(drawn.shape))
    spots = []
    for shift in (0, 1):
        where = [jax.random.randint(jax.random.fold_in(stream_key, axis), (), 0, length) for axis, length in enumerate(drawn.shape)]
        where[longest] = (where[longest] + shift) % drawn.shape[longest]
        spots.append(tuple(where))
    return drawn.at[spots[0]].set(smallest).at[spots[1]].set(largest)


def level_of(own_key, dims, cuts, smallest, largest):
    def one(axis_at, parts):
        heights = jax.random.uniform(jax.random.fold_in(jax.random.fold_in(own_key, 6), axis_at), (parts,), jnp.float32, smallest / len(cuts), largest / len(cuts))
        return jnp.repeat(jnp.exp(heights), dims[axis_at] // parts).reshape((-1,) + (1,) * (len(dims) - axis_at - 1))

    gain = one(*cuts[0])
    for cut in cuts[1:]:
        gain = gain * one(*cut)
    return gain


def noise(stream_key, shape, deviation, bound, pieces=(), kind=jnp.bfloat16):
    values = deviation * jax.random.normal(stream_key, shape, jnp.float32)
    if pieces:
        values = values * level_of(stream_key, shape, pieces, -0.22, 0.18)
    return jnp.clip(values, -bound, bound).astype(kind)


def setup_inputs(seed: int = 0) -> dict:
    key_list = jax.random.split(jax.random.key(seed), 10)
    tracers = draw_tracers(jax.random.fold_in(key_list[9], 71), 0)
    east_velocity = noise(key_list[1], (LEV, NY, NX), 0.2, 0.6, ((0, 4), (1, 4), (2, 16)), jnp.float32)
    north_velocity = noise(key_list[2], (LEV, NY, NX), 0.2, 0.6, ((0, 4), (1, 4), (2, 16)), jnp.float32)
    surface = noise(key_list[3], (NY, NX), 0.3, 1.5, ((0, 4), (1, 16)), jnp.float32)
    depth = jnp.clip(1.0 + 2.0 * jax.random.uniform(key_list[4], (NY, NX), jnp.float32) ** level_of(key_list[4], (NY, NX), ((0, 4), (1, 16)), -0.2, 0.2), 1.0, 3.0)
    wet_mask = plant((jax.random.randint(key_list[5], (NY, NX), 0, 8) < 7).astype(jnp.int32), jax.random.fold_in(key_list[5], 1), 0, 1)
    river_cells = plant(jax.random.randint(key_list[6], (RIVERS,), 0, CY * CX), jax.random.fold_in(key_list[6], 1), 0, (CY * CX) - 1).astype(jnp.int32)
    river_loads = jnp.clip(0.2 + 1.8 * jax.random.uniform(key_list[7], (RIVERS, NTR), jnp.float32) ** level_of(key_list[7], (RIVERS, NTR), ((0, 64),), -0.2, 0.2), 0.2, 2.0)
    kinetics = draw_kinetics(jax.random.fold_in(key_list[9], 71), 0)
    return {"tracers": tracers, "east_velocity": east_velocity, "north_velocity": north_velocity, "surface": surface, "depth": depth, "wet_mask": wet_mask, "river_cells": river_cells, "river_loads": river_loads, "kinetics": kinetics}


eta_rate = 0.25
gravity_rate = 0.25
baroclinic_rate = 0.4
viscous_rate = 0.1
friction_rate = 0.3
advect_rate = 0.3
mixing_rate = 0.2
haline_coef = 0.8
thermal_coef = 0.2
warming_rate = 0.46


def face_terms(depth_pad, wet_pad):
    east_open = wet_pad[:, :-1] * wet_pad[:, 1:]
    north_open = wet_pad[:-1, :] * wet_pad[1:, :]
    east_depth = 0.5 * (depth_pad[:, :-1] + depth_pad[:, 1:]) * east_open
    north_depth = 0.5 * (depth_pad[:-1, :] + depth_pad[1:, :]) * north_open
    return east_open, north_open, east_depth, north_depth


def laplace(field_pad):
    inner = field_pad[:, 1:-1, 1:-1]
    return (field_pad[:, 2:, 1:-1] + field_pad[:, :-2, 1:-1] + field_pad[:, 1:-1, 2:]
            + field_pad[:, 1:-1, :-2] - 4.0 * inner)


def advect(tracer_pad, east_flux, north_flux, depth, levels):
    east_speed = east_flux[:, 1:-1, :]
    east_term = (jnp.maximum(east_speed, 0.0) * tracer_pad[..., 1:-1, :-1]
                 + jnp.minimum(east_speed, 0.0) * tracer_pad[..., 1:-1, 1:])
    north_speed = north_flux[:, :, 1:-1]
    north_term = (jnp.maximum(north_speed, 0.0) * tracer_pad[..., :-1, 1:-1]
                  + jnp.minimum(north_speed, 0.0) * tracer_pad[..., 1:, 1:-1])
    divergence = (east_term[..., 1:] - east_term[..., :-1]
                  + north_term[..., 1:, :] - north_term[..., :-1, :])
    return tracer_pad[..., 1:-1, 1:-1] - advect_rate * levels * divergence / depth


def vertical_mix(advected, level_above, level_below, has_above, has_below):
    return advected + mixing_rate * (has_above * (level_above - advected)
                                     + has_below * (level_below - advected))


def pad_plane(field):
    return jnp.pad(field, ((1, 1), (1, 1)))


def pad_levels(field):
    return jnp.pad(field, ((0, 0), (1, 1), (1, 1)))


def reference(tracers, east_velocity, north_velocity, surface, depth, wet_mask, river_cells, river_loads, kinetics):
    levels = tracers.shape[1]
    wet_cells = wet_mask.astype(jnp.float32)
    east_open, north_open, east_depth, north_depth = face_terms(pad_plane(depth), pad_plane(wet_cells))
    east_pad = pad_levels(east_velocity)
    north_pad = pad_levels(north_velocity)
    east_flux = east_pad[:, :, :-1] * east_depth / levels
    north_flux = north_pad[:, :-1, :] * north_depth / levels
    column_east = jnp.sum(east_flux, 0)
    column_north = jnp.sum(north_flux, 0)
    divergence = (column_east[1:-1, 1:] - column_east[1:-1, :-1]
                  + column_north[1:, 1:-1] - column_north[:-1, 1:-1])
    new_surface = surface - eta_rate * wet_cells * divergence
    density = haline_coef * tracers[0] - thermal_coef * tracers[1]
    pressure = baroclinic_rate * depth * (jnp.cumsum(density, 0) - 0.5 * density) / levels
    pressure_pad = pad_levels(pressure)
    surface_pad = pad_plane(new_surface)
    level_index = jnp.arange(levels, dtype=jnp.int32)
    bottom = (level_index == levels - 1).astype(jnp.float32)[:, None, None]
    new_east = east_open[1:-1, 1:] * (
        east_velocity - gravity_rate * (surface_pad[1:-1, 2:] - surface_pad[1:-1, 1:-1])
        - (pressure_pad[:, 1:-1, 2:] - pressure_pad[:, 1:-1, 1:-1])
        + viscous_rate * laplace(east_pad) - friction_rate * bottom * east_velocity)
    new_north = north_open[1:, 1:-1] * (
        north_velocity - gravity_rate * (surface_pad[2:, 1:-1] - surface_pad[1:-1, 1:-1])
        - (pressure_pad[:, 2:, 1:-1] - pressure_pad[:, 1:-1, 1:-1])
        + viscous_rate * laplace(north_pad) - friction_rate * bottom * north_velocity)
    has_above = (level_index > 0).astype(jnp.float32)[:, None, None]
    has_below = (level_index < levels - 1).astype(jnp.float32)[:, None, None]

    def one_tracer(field):
        advected = advect(pad_levels(field), east_flux, north_flux, depth, levels)
        zero_level = jnp.zeros_like(advected[:1])
        level_above = jnp.concatenate([zero_level, advected[:-1]], 0)
        level_below = jnp.concatenate([advected[1:], zero_level], 0)
        blended = vertical_mix(advected, level_above, level_below, has_above, has_below)
        return field + wet_cells * (blended - field)

    updated = lax.map(one_tracer, tracers)
    warming = jnp.exp(warming_rate * updated[1])
    reaction = jnp.einsum('ab,blyx->alyx', kinetics, updated, precision=lax.Precision.HIGHEST)
    river_index = jnp.arange(river_cells.shape[0], dtype=jnp.int32)
    tile = river_index // RIV_DEV
    river_rows = (tile // N_TX) * CY + river_cells // CX
    river_cols = (tile % N_TX) * CX + river_cells % CX
    source = jnp.zeros((tracers.shape[0],) + depth.shape, jnp.float32)
    source = source.at[:, river_rows, river_cols].add(river_loads.T)
    level_top = (level_index == 0).astype(jnp.float32)[:, None, None]
    new_tracers = updated + wet_cells * (warming * reaction + level_top * source[:, None])
    return new_tracers, new_east, new_north, new_surface
```

```python
import functools

import jax
import jax.numpy as jnp
from jax import lax
from jax.experimental import pallas as pl
from jax.experimental.pallas import tpu as pltpu
from jax.sharding import PartitionSpec as P

f32 = jnp.float32
MESH = pl.DeviceIdType.MESH

eta_rate = 0.25
gravity_rate = 0.25
baroclinic_rate = 0.4
viscous_rate = 0.1
friction_rate = 0.3
advect_rate = 0.3
mixing_rate = 0.2
haline_coef = 0.8
thermal_coef = 0.2
warming_rate = 0.46

PAD = 8
BULK_FIRST = 4
BULK_SECOND = 6
BULK_THIRD = 10


def step_kernel(
    levels,
    tr_hbm, u_hbm, v_hbm, sf_hbm, dp_hbm, wm_hbm, rc_hbm, rl_hbm, kin_hbm,
    out_tr, out_u, out_v, out_s,
    trp, up, vp, sfb, dpp, wmb, wp, kb,
    fb, gp, sb, spb, srecv, db, dpb, drecv,
    ns_send, ns_recv, q, ew_recv, mb,
    xb, xt, xr, yb, bx, adv, ga, gb,
    nsp, pp, c2, c2t, e2, t2, r2, n2,
    rc, rl, kin, load_sem, halo_ss, halo_rs, red_ss, red_rs, x_ss, x_rs, p2_ss, p2_rs, bulk_ss, bulk_rs,
):
    g, gy, gt = lax.axis_index("grp"), lax.axis_index("ty"), lax.axis_index("tx")
    n_grp, n_ty, n_tx = lax.axis_size("grp"), lax.axis_size("ty"), lax.axis_size("tx")
    nt = tr_hbm.shape[0]
    rows, lanes = sfb.shape
    blocks = rows // 8
    n_uv = 2 * nt
    f_d, f_w = n_uv + 4, n_uv + 5

    up_there, down_there = g > 0, g < n_grp - 1
    first = g + 1 - 2 * lax.rem(g, 2)
    second = n_grp - 1 - g

    lane = lax.broadcasted_iota(jnp.int32, (8, lanes), 1)
    sub = lax.broadcasted_iota(jnp.int32, (8, lanes), 0)
    pair = lane // 2
    even = lax.rem(lane, 2) == 0
    at_east, at_west = lane == lanes - 1, lane == 0
    at_edge = jnp.logical_or(at_east, at_west)

    def roll(x, shift):
        shift = shift % lanes
        return x if shift == 0 else pltpu.roll(x, shift, 1)

    def unpacked(tile, field):
        return roll(tile, lanes - 1 - 2 * field)

    def blk(r):
        return pl.ds(pl.multiple_of(r * 8, 8), 8)

    def mid(r):
        return pl.ds(pl.multiple_of(r * 8 + PAD, 8), 8)

    def south(r):
        return pl.ds(r * 8 + (PAD - 1), 8)

    def north(r):
        return pl.ds(r * 8 + (PAD + 1), 8)

    inner = pl.ds(PAD, rows)
    loads = [
        pltpu.make_async_copy(u_hbm, up.at[:, inner, :], load_sem.at[0]),
        pltpu.make_async_copy(v_hbm, vp.at[:, inner, :], load_sem.at[1]),
        pltpu.make_async_copy(dp_hbm, dpp.at[inner, :], load_sem.at[2]),
        pltpu.make_async_copy(wm_hbm, wmb, load_sem.at[3]),
        pltpu.make_async_copy(tr_hbm, trp.at[:, :, inner, :], load_sem.at[4]),
        pltpu.make_async_copy(sf_hbm, sfb, load_sem.at[5]),
        pltpu.make_async_copy(kin_hbm, kin, load_sem.at[6]),
        pltpu.make_async_copy(rc_hbm, rc, load_sem.at[7]),
        pltpu.make_async_copy(rl_hbm, rl, load_sem.at[8]),
    ]
    for load in loads:
        load.start()

    neighbours = [
        (None, {"grp": first}),
        (None, {"grp": second}),
        (gy > 0, {"ty": gy - 1}),
        (gy < n_ty - 1, {"ty": gy + 1}),
        (gt > 0, {"tx": gt - 1}),
        (gt < n_tx - 1, {"tx": gt + 1}),
    ]
    barrier = pltpu.get_barrier_semaphore()
    for there, device in neighbours:
        if there is None:
            pl.semaphore_signal(barrier, inc=1, device_id=device, device_id_type=MESH)
        else:

            @pl.when(there)
            def _(device=device):
                pl.semaphore_signal(barrier, inc=1, device_id=device, device_id_type=MESH)

    def remote(src, dst, ss, rs, device):
        return pltpu.make_async_remote_copy(
            src_ref=src, dst_ref=dst, send_sem=ss, recv_sem=rs, device_id=device, device_id_type=MESH
        )

    to_north = remote(ns_send.at[0], ns_recv.at[0], halo_ss.at[0], halo_rs.at[0], {"ty": gy + 1})
    to_south = remote(ns_send.at[1], ns_recv.at[1], halo_ss.at[1], halo_rs.at[1], {"ty": gy - 1})
    to_east = remote(q, ew_recv.at[0], halo_ss.at[2], halo_rs.at[2], {"tx": gt + 1})
    to_west = remote(q, ew_recv.at[1], halo_ss.at[3], halo_rs.at[3], {"tx": gt - 1})
    halo_sends = [
        (gy < n_ty - 1, to_north),
        (gy > 0, to_south),
        (gt < n_tx - 1, to_east),
        (gt > 0, to_west),
    ]
    halo_recvs = [
        (gy > 0, to_north),
        (gy < n_ty - 1, to_south),
        (gt > 0, to_east),
        (gt < n_tx - 1, to_west),
    ]
    s_first = remote(sb, srecv.at[0], red_ss.at[0], red_rs.at[0], {"grp": first})
    s_second = remote(spb, srecv.at[1], red_ss.at[1], red_rs.at[1], {"grp": second})
    d_first = remote(db, drecv.at[0], red_ss.at[2], red_rs.at[2], {"grp": first})
    d_second = remote(dpb, drecv.at[1], red_ss.at[3], red_rs.at[3], {"grp": second})
    low, high = pl.ds(0, 2 * nt), pl.ds(2 * nt, 2 * nt)
    x_up = remote(xt.at[low, :], xr.at[high, :], x_ss.at[0], x_rs.at[0], {"grp": g - 1})
    x_down = remote(xt.at[high, :], xr.at[low, :], x_ss.at[1], x_rs.at[1], {"grp": g + 1})
    p2_west = remote(
        c2t.at[pl.ds(0, 8), :], e2.at[pl.ds(0, 8), :], p2_ss.at[0], p2_rs.at[0], {"tx": gt - 1}
    )
    p2_south = remote(r2, n2, p2_ss.at[1], p2_rs.at[1], {"ty": gy - 1})

    def bulk_up(r):
        return remote(adv.at[0, r], gb.at[r], bulk_ss.at[0, r], bulk_rs.at[0, r], {"grp": g - 1})

    def bulk_down(r):
        return remote(adv.at[1, r], ga.at[r], bulk_ss.at[1, r], bulk_rs.at[1, r], {"grp": g + 1})

    def send_bulk(r):
        @pl.when(up_there)
        def _():
            bulk_up(r).start()

        @pl.when(down_there)
        def _():
            bulk_down(r).start()

    def loop(start, stop, body):
        lax.fori_loop(start, stop, lambda i, c: (body(i), c)[1], 0)

    zero = jnp.zeros((8, lanes), f32)

    def clear(ref):
        def one(i):
            ref[blk(i), :] = zero

        loop(0, ref.shape[0] // 8, one)

    def clear_ghost(ref):
        def one(i):
            for n in range(nt):
                ref[i, n] = zero

        loop(0, blocks, one)

    @pl.when(jnp.logical_not(up_there))
    def _():
        clear_ghost(ga)
        clear(xr.at[low, :])

    @pl.when(jnp.logical_not(down_there))
    def _():
        clear_ghost(gb)
        clear(xr.at[high, :])

    clear(xr.at[pl.ds(4 * nt, lanes - 4 * nt), :])
    clear(e2.at[pl.ds(8, lanes - 8), :])

    for slot, (there, _) in enumerate(halo_recvs):

        @pl.when(jnp.logical_not(there))
        def _(slot=slot):
            clear(ns_recv.at[slot] if slot < 2 else ew_recv.at[slot - 2])

    @pl.when(gt == n_tx - 1)
    def _():
        e2[pl.ds(0, 8), :] = zero

    @pl.when(gy == n_ty - 1)
    def _():
        n2[...] = zero

    for load in loads[:4]:
        load.wait()
    for edge in (0, PAD + rows):
        dpp[pl.ds(edge, 8), :] = zero
        wp[pl.ds(edge, 8), :] = zero

    def wetness(r):
        wp[mid(r), :] = wmb[blk(r), :].astype(f32)

    loop(0, blocks, wetness)

    def north_face(r):
        d, w = dpp[mid(r), :], wp[mid(r), :]
        depth_n = (0.5 / levels) * (d + dpp[north(r), :]) * (w * wp[north(r), :])
        for l in range(2):
            gp[l, mid(r), :] = vp[l, mid(r), :] * depth_n

    def faces(r):
        d, w = dpp[mid(r), :], wp[mid(r), :]
        depth_e = (0.5 / levels) * (d + roll(d, -1)) * (w * roll(w, -1))
        depth_e = jnp.where(at_east, 0.0, depth_e)
        for l in range(2):
            fb[l, blk(r), :] = up[l, mid(r), :] * depth_e
        north_face(r)

    loop(0, blocks, faces)
    loads[4].wait()

    def edges(r):
        sb[blk(r), :] = haline_coef * (trp[0, 0, mid(r), :] + trp[0, 1, mid(r), :]) - thermal_coef * (
            trp[1, 0, mid(r), :] + trp[1, 1, mid(r), :]
        )
        packed = zero
        fields = [trp[n, l, mid(r), :] for l in range(2) for n in range(nt)]
        fields += [up[0, mid(r), :], up[1, mid(r), :], vp[0, mid(r), :], vp[1, mid(r), :]]
        fields += [dpp[mid(r), :], wp[mid(r), :]]
        for f, field in enumerate(fields):
            packed = jnp.where(pair == f, roll(field, 2 * f + 1), packed)
        q[blk(r), :] = packed

    loop(0, blocks, edges)

    padded = [trp.at[n, l] for l in range(2) for n in range(nt)]
    padded += [up.at[0], up.at[1], vp.at[0], vp.at[1], dpp, wp]
    for f, ref in enumerate(padded):
        ns_send[0, pl.ds(f, 1), :] = ref[pl.ds(PAD + rows - 1, 1), :]
        ns_send[1, pl.ds(f, 1), :] = ref[pl.ds(PAD, 1), :]
    for f in range(len(padded), ns_send.shape[1]):
        for slot in range(2):
            ns_send[slot, pl.ds(f, 1), :] = jnp.zeros((1, lanes), f32)

    peers = sum(1 if there is None else there.astype(jnp.int32) for there, _ in neighbours)
    pl.semaphore_wait(barrier, peers)

    s_first.start()
    for there, copy in reversed(halo_sends):

        @pl.when(there)
        def _(copy=copy):
            copy.start()

    def advect(r):
        d = dpp[mid(r), :]
        scale = (advect_rate * levels) / d
        for l in range(2):
            fe, gn, gs = fb[l, blk(r), :], gp[l, mid(r), :], gp[l, south(r), :]
            fw = roll(fe, 1)
            out = (jnp.maximum(fe, 0.0) - jnp.minimum(fw, 0.0)) + (
                jnp.maximum(gn, 0.0) - jnp.minimum(gs, 0.0)
            )
            own = 1.0 - scale * out
            from_e, from_w = -scale * jnp.minimum(fe, 0.0), scale * jnp.maximum(fw, 0.0)
            from_n, from_s = -scale * jnp.minimum(gn, 0.0), scale * jnp.maximum(gs, 0.0)
            for n in range(nt):
                c = trp[n, l, mid(r), :]
                adv[l, r, n] = (
                    (own * c + from_e * roll(c, -1))
                    + (from_w * roll(c, 1) + from_n * trp[n, l, north(r), :])
                    + from_s * trp[n, l, south(r), :]
                )

    def advect_and_send(r):
        advect(r)

        @pl.when(jnp.logical_and(r > 1, r <= BULK_FIRST + 1))
        def _():
            send_bulk(r - 1)

    loop(1, blocks - 1, advect_and_send)

    s_first.wait_recv()

    def pair_density(r):
        spb[blk(r), :] = sb[blk(r), :] + srecv[0, blk(r), :]

    loop(0, blocks, pair_density)

    for load in loads[5:]:
        load.wait()

    def spread(n):
        for m in range(nt):
            kb[n, m] = jnp.full((8, lanes), kin[n, m], f32)

    loop(0, nt, spread)

    for there, copy in halo_recvs:

        @pl.when(there)
        def _(copy=copy):
            copy.wait_recv()

    s_second.start()

    for f, ref in enumerate(padded):
        ref[pl.ds(PAD - 1, 1), :] = ns_recv[0, pl.ds(f, 1), :]
        ref[pl.ds(PAD + rows, 1), :] = ns_recv[1, pl.ds(f, 1), :]
    d_south, w_south = dpp[pl.ds(PAD - 1, 1), :], wp[pl.ds(PAD - 1, 1), :]
    d_row, w_row = dpp[pl.ds(PAD, 1), :], wp[pl.ds(PAD, 1), :]
    depth_s = (0.5 / levels) * (d_south + d_row) * (w_south * w_row)
    for l in range(2):
        gp[l, pl.ds(PAD - 1, 1), :] = vp[l, pl.ds(PAD - 1, 1), :] * depth_s
    north_face(blocks - 1)

    def rim(r):
        m = jnp.where(even, roll(ew_recv[1, blk(r), :], -1), roll(ew_recv[0, blk(r), :], 1))
        mb[blk(r), :] = m
        d, w = dpp[mid(r), :], wp[mid(r), :]
        scale = (advect_rate * levels) / d
        depth_f = (0.5 / levels) * (d + unpacked(m, f_d)) * (w * unpacked(m, f_w))
        total = zero
        parts = []
        for l in range(2):
            flow = jnp.where(at_west, unpacked(m, n_uv + l), up[l, mid(r), :])
            flux = jnp.where(at_edge, flow * depth_f, 0.0)
            fe = fb[l, blk(r), :]
            total = total + (
                (fe - roll(fe, 1))
                + (gp[l, mid(r), :] - gp[l, south(r), :])
                + jnp.where(at_east, flux, -flux)
            )
            z = scale * flux
            z_e = jnp.broadcast_to(z[:, lanes - 1 : lanes], (8, lanes))
            z_w = jnp.broadcast_to(z[:, 0:1], (8, lanes))
            parts.append(jnp.where(even, -z_e, z_w))
        db[blk(r), :] = total
        zz = jnp.where(lane < 2 * nt, parts[0], parts[1])
        xb[blk(r), :] = jnp.minimum(zz, 0.0) * q[blk(r), :] + jnp.maximum(zz, 0.0) * m

    loop(0, blocks, rim)
    xt[...] = jnp.transpose(xb[...])
    advect(0)
    d_first.start()

    @pl.when(up_there)
    def _():
        x_up.start()

    @pl.when(down_there)
    def _():
        x_down.start()

    loop(BULK_FIRST + 1, BULK_SECOND + 1, send_bulk)
    advect(blocks - 1)

    d_first.wait_recv()

    def pair_divergence(r):
        dpb[blk(r), :] = db[blk(r), :] + drecv[0, blk(r), :]

    loop(0, blocks, pair_divergence)
    s_second.wait_recv()

    over_first = (lax.rem(g, 2) == 1).astype(f32)
    over_second = (g >= 2).astype(f32)
    press = baroclinic_rate / levels

    def pressure(r):
        over = over_first * srecv[0, blk(r), :] + over_second * srecv[1, blk(r), :]
        dens = [
            haline_coef * trp[0, l, mid(r), :] - thermal_coef * trp[1, l, mid(r), :] for l in range(2)
        ]
        d = press * dpp[mid(r), :]
        pp[0, blk(r), :] = d * (over + 0.5 * dens[0])
        pp[1, blk(r), :] = d * (over + dens[0] + 0.5 * dens[1])

    loop(0, blocks, pressure)
    d_second.start()
    loop(BULK_SECOND + 1, BULK_THIRD + 1, send_bulk)

    @pl.when(up_there)
    def _():
        x_down.wait_recv()

    @pl.when(down_there)
    def _():
        x_up.wait_recv()

    yb[...] = jnp.transpose(xr[...])
    mix_up = jnp.where(up_there, mixing_rate, 0.0).astype(f32)
    mix_down = jnp.where(down_there, mixing_rate, 0.0).astype(f32)
    own_up = (1.0 - mixing_rate) - mix_up
    own_down = (1.0 - mixing_rate) - mix_down

    def blend_edges(r):
        x = xb[blk(r), :]
        is_top = lane < 2 * nt
        other = jnp.where(is_top, roll(x, -2 * nt), roll(x, 2 * nt))
        bx[blk(r), :] = (
            jnp.where(is_top, own_up, own_down) * x
            + mixing_rate * other
            + jnp.where(is_top, mix_up, mix_down) * yb[blk(r), :]
        )

    loop(0, blocks, blend_edges)

    d_second.wait_recv()

    def surface(r):
        ns = sfb[blk(r), :] - eta_rate * wp[mid(r), :] * (dpb[blk(r), :] + drecv[1, blk(r), :])
        out_s[blk(r), :] = ns
        nsp[blk(r), :] = ns
        p0, p1 = pp[0, blk(r), :], pp[1, blk(r), :]
        c2[blk(r), :] = jnp.where(
            lane == 0, ns, jnp.where(lane == 1, roll(p0, 1), jnp.where(lane == 2, roll(p1, 2), 0.0))
        )

    loop(0, blocks, surface)
    r2[...] = zero
    r2[pl.ds(0, 1), :] = nsp[pl.ds(0, 1), :]
    for l in range(2):
        r2[pl.ds(1 + l, 1), :] = pp[l, pl.ds(0, 1), :]
    c2t[...] = jnp.transpose(c2[...])

    loop(BULK_THIRD + 1, blocks - 1, send_bulk)
    loop(0, 2, lambda i: send_bulk(i * (blocks - 1)))

    @pl.when(gt > 0)
    def _():
        p2_west.start()

    @pl.when(gy > 0)
    def _():
        p2_south.start()

    is_top_level = (g == 0).astype(f32)

    def finish(r):
        @pl.when(up_there)
        def _():
            bulk_down(r).wait_recv()

        @pl.when(down_there)
        def _():
            bulk_up(r).wait_recv()

        w = wp[mid(r), :]
        edge = bx[blk(r), :]
        updated = [[], []]
        for n in range(nt):
            a0, a1 = adv[0, r, n], adv[1, r, n]
            e0 = jnp.where(at_edge, unpacked(edge, n), 0.0)
            e1 = jnp.where(at_edge, unpacked(edge, nt + n), 0.0)
            b0 = (own_up * a0 + mixing_rate * a1) + (mix_up * ga[r, n] + e0)
            b1 = (own_down * a1 + mixing_rate * a0) + (mix_down * gb[r, n] + e1)
            for l, b in enumerate((b0, b1)):
                c = trp[n, l, mid(r), :]
                updated[l].append(c + w * (b - c))
        warm = [w * jnp.exp(warming_rate * updated[l][1]) for l in range(2)]
        cell = (r * 8 + sub) * lanes + lane
        top = is_top_level * w
        hits = [jnp.where(cell == rc[i], top, 0.0) for i in range(rc.shape[0])]
        for n in range(nt):
            k = kb[n, 0]
            react = [k * updated[l][0] for l in range(2)]
            for m in range(1, nt):
                k = kb[n, m]
                react = [react[l] + k * updated[l][m] for l in range(2)]
            source = hits[0] * rl[0, n]
            for i in range(1, rc.shape[0]):
                source = source + hits[i] * rl[i, n]
            out_tr[n, 0, blk(r), :] = updated[0][n] + (warm[0] * react[0] + source)
            out_tr[n, 1, blk(r), :] = updated[1][n] + warm[1] * react[1]

    half = blocks // 2
    loop(1, half + 1, finish)

    @pl.when(gt < n_tx - 1)
    def _():
        p2_west.wait_recv()

    @pl.when(gy < n_ty - 1)
    def _():
        p2_south.wait_recv()

    t2[...] = jnp.transpose(e2[...])
    nsp[pl.ds(rows, 1), :] = n2[pl.ds(0, 1), :]
    for l in range(2):
        pp[l, pl.ds(rows, 1), :] = n2[pl.ds(1 + l, 1), :]
    friction = jnp.where(g == n_grp - 1, friction_rate, 0.0).astype(f32)

    def velocities(r):
        m = mb[blk(r), :]
        t = t2[blk(r), :]
        w = wp[mid(r), :]
        open_e = w * jnp.where(at_east, unpacked(m, f_w), roll(w, -1))
        open_n = w * wp[north(r), :]
        above = pl.ds(r * 8 + 1, 8)
        ns = nsp[blk(r), :]
        slope_e = jnp.where(at_east, roll(t, -1), roll(ns, -1)) - ns
        slope_n = nsp[above, :] - ns
        for l in range(2):
            p = pp[l, blk(r), :]
            push_e = jnp.where(at_east, roll(t, -2 - l), roll(p, -1)) - p
            push_n = pp[l, above, :] - p
            for ref, out, field, opened, slope, push in (
                (up, out_u, n_uv + l, open_e, slope_e, push_e),
                (vp, out_v, n_uv + 2 + l, open_n, slope_n, push_n),
            ):
                x = ref[l, mid(r), :]
                beside = unpacked(m, field)
                lap = (
                    (ref[l, north(r), :] + ref[l, south(r), :])
                    + (jnp.where(at_east, beside, roll(x, -1)) + jnp.where(at_west, beside, roll(x, 1)))
                    - 4.0 * x
                )
                new = x - gravity_rate * slope - push + viscous_rate * lap
                if l == 1:
                    new = new - friction * x
                out[l, blk(r), :] = opened * new

    loop(0, blocks, velocities)
    loop(half + 1, blocks - 1, finish)
    loop(0, 2, lambda i: finish(i * (blocks - 1)))

    for copy in (s_first, s_second, d_first, d_second):
        copy.wait_send()
    for there, copy in halo_sends + [
        (up_there, x_up),
        (down_there, x_down),
        (gt > 0, p2_west),
        (gy > 0, p2_south),
    ]:

        @pl.when(there)
        def _(copy=copy):
            copy.wait_send()

    def sent(r):
        @pl.when(up_there)
        def _():
            bulk_up(r).wait_send()

        @pl.when(down_there)
        def _():
            bulk_down(r).wait_send()

    loop(0, blocks, sent)


def put_kernel(*refs):
    sources, targets, sem = refs[:4], refs[4:8], refs[8]
    puts = [pltpu.make_async_copy(a, b, sem.at[i]) for i, (a, b) in enumerate(zip(sources, targets))]
    for put in puts:
        put.start()
    for put in puts:
        put.wait()


def shards(tracers, east_velocity, north_velocity, surface, depth, wet_mask, river_cells, river_loads, kinetics):
    nt, own, rows, lanes = tracers.shape
    levels = own * lax.axis_size("grp")
    blocks = rows // 8
    tall = rows + 2 * PAD
    tile = pltpu.VMEM((rows, lanes), f32)
    twice = pltpu.VMEM((2, rows, lanes), f32)
    edges = pltpu.VMEM((2, 40, lanes), f32)
    dma = pltpu.SemaphoreType.DMA
    scratch = [
        pltpu.VMEM((nt, 2, tall, lanes), f32),
        pltpu.VMEM((2, tall, lanes), f32),
        pltpu.VMEM((2, tall, lanes), f32),
        tile,
        pltpu.VMEM((tall, lanes), f32),
        pltpu.VMEM((rows, lanes), jnp.int32),
        pltpu.VMEM((tall, lanes), f32),
        pltpu.VMEM((nt, nt, 8, lanes), f32),
        twice,
        pltpu.VMEM((2, tall, lanes), f32),
        tile,
        tile,
        twice,
        tile,
        tile,
        twice,
        edges,
        edges,
        tile,
        twice,
        tile,
        tile,
        tile,
        tile,
        tile,
        tile,
        pltpu.VMEM((2, blocks, nt, 8, lanes), f32),
        pltpu.VMEM((blocks, nt, 8, lanes), f32),
        pltpu.VMEM((blocks, nt, 8, lanes), f32),
        pltpu.VMEM((rows + 8, lanes), f32),
        pltpu.VMEM((2, rows + 8, lanes), f32),
        tile,
        tile,
        tile,
        tile,
        pltpu.VMEM((8, lanes), f32),
        pltpu.VMEM((8, lanes), f32),
        pltpu.SMEM(river_cells.shape, jnp.int32),
        pltpu.SMEM(river_loads.shape, f32),
        pltpu.SMEM((nt, nt), f32),
        dma((9,)),
        dma((4,)),
        dma((4,)),
        dma((4,)),
        dma((4,)),
        dma((2,)),
        dma((2,)),
        dma((2,)),
        dma((2,)),
        dma((2, blocks)),
        dma((2, blocks)),
    ]
    anywhere = pl.BlockSpec(memory_space=pltpu.HBM)
    vmem = pl.BlockSpec(memory_space=pltpu.VMEM)
    outs = (
        jax.ShapeDtypeStruct(tracers.shape, f32),
        jax.ShapeDtypeStruct(east_velocity.shape, f32),
        jax.ShapeDtypeStruct(north_velocity.shape, f32),
        jax.ShapeDtypeStruct(surface.shape, f32),
    )
    fields = [
        pltpu.with_memory_space_constraint(x, pltpu.HBM)
        for x in (
            tracers, east_velocity, north_velocity, surface, depth, wet_mask,
            river_cells, river_loads, kinetics,
        )
    ]
    results = pl.pallas_call(
        functools.partial(step_kernel, levels),
        out_shape=outs,
        in_specs=[anywhere] * 9,
        out_specs=(vmem,) * 4,
        scratch_shapes=scratch,
        compiler_params=pltpu.CompilerParams(
            collective_id=0, has_side_effects=True, vmem_limit_bytes=32 * 1024 * 1024
        ),
        name="estuary_step",
    )(*fields)
    return pl.pallas_call(
        put_kernel,
        out_shape=outs,
        in_specs=[pl.BlockSpec(memory_space=pl.ANY)] * 4,
        out_specs=(pl.BlockSpec(memory_space=pl.ANY),) * 4,
        scratch_shapes=[dma((4,))],
        compiler_params=pltpu.CompilerParams(vmem_limit_bytes=1024 * 1024),
        name="put",
    )(*results)


def solution(mesh):
    return jax.shard_map(
        shards,
        mesh=mesh,
        in_specs=(
            P(None, "grp", "ty", "tx"),
            P("grp", "ty", "tx"),
            P("grp", "ty", "tx"),
            P("ty", "tx"),
            P("ty", "tx"),
            P("ty", "tx"),
            P(("ty", "tx")),
            P(("ty", "tx"), None),
            P(),
        ),
        out_specs=(
            P(None, "grp", "ty", "tx"),
            P("grp", "ty", "tx"),
            P("grp", "ty", "tx"),
            P("ty", "tx"),
        ),
        check_vma=False,
    )
```

```python
import functools

import jax
import jax.numpy as jnp
from jax import lax
from jax.experimental import pallas as pl
from jax.experimental.pallas import tpu as pltpu
from jax.sharding import PartitionSpec as P

f32 = jnp.float32
MESH = pl.DeviceIdType.MESH

eta_rate = 0.25
gravity_rate = 0.25
baroclinic_rate = 0.4
viscous_rate = 0.1
friction_rate = 0.3
advect_rate = 0.3
mixing_rate = 0.2
haline_coef = 0.8
thermal_coef = 0.2
warming_rate = 0.46

PAD = 8
TALL = 32
BULK_FIRST = 2
VELOCITIES_AFTER = 5


def step_kernel(
    levels,
    tr_hbm, u_hbm, v_hbm, sf_hbm, dp_hbm, wm_hbm, rc_hbm, rl_hbm, kin_hbm,
    out_tr, out_u, out_v, out_s,
    trp, up, vp, sfb, dpp, wmb, wp, kb,
    fb, gp, sdb, sdp, sdr,
    ns_send, ns_recv, q, qt, ew_send, ew_recv, mt, mb,
    xb, xt, xr, er, yb, bx, adv, ga, gb,
    nsp, pp, c2, c2t, e2, t2, r2, n2,
    rc, rl, kin, load_sem, halo_ss, halo_rs, red_ss, red_rs, e_ss, e_rs, x_ss, x_rs, p2_ss, p2_rs, bulk_ss, bulk_rs,
):
    g, gy, gt = lax.axis_index("grp"), lax.axis_index("ty"), lax.axis_index("tx")
    n_grp, n_ty, n_tx = lax.axis_size("grp"), lax.axis_size("ty"), lax.axis_size("tx")
    nt = tr_hbm.shape[0]
    rows, lanes = sfb.shape
    blocks = rows // 8
    n_uv = 2 * nt
    f_d, f_w = n_uv + 4, n_uv + 5

    up_there, down_there = g > 0, g < n_grp - 1
    first = g + 1 - 2 * lax.rem(g, 2)
    second = n_grp - 1 - g
    third = lax.rem(g + n_grp // 2, n_grp)

    lane = lax.broadcasted_iota(jnp.int32, (8, lanes), 1)
    sub = lax.broadcasted_iota(jnp.int32, (8, lanes), 0)
    short_edge = jnp.logical_or(lane == lanes - 1, lane == 0)
    lane_t = lax.broadcasted_iota(jnp.int32, (TALL, lanes), 1)
    sub_t = lax.broadcasted_iota(jnp.int32, (TALL, lanes), 0)
    pair = lane_t // 2
    even = lax.rem(lane_t, 2) == 0
    at_east, at_west = lane_t == lanes - 1, lane_t == 0
    at_edge = jnp.logical_or(at_east, at_west)

    def roll(x, shift):
        shift = shift % lanes
        return x if shift == 0 else pltpu.roll(x, shift, 1)

    def unpacked(tile, field):
        return roll(tile, lanes - 1 - 2 * field)

    def blk(r):
        return pl.ds(pl.multiple_of(r * 8, 8), 8)

    def tall(i):
        return pl.ds(pl.multiple_of(i * TALL, TALL), TALL)

    def mid(r, n=8):
        return pl.ds(pl.multiple_of(r * n + PAD, 8), n)

    def south(r, n=8):
        return pl.ds(r * n + (PAD - 1), n)

    def north(r, n=8):
        return pl.ds(r * n + (PAD + 1), n)

    inner = pl.ds(PAD, rows)
    loads = [
        pltpu.make_async_copy(u_hbm, up.at[:, inner, :], load_sem.at[0]),
        pltpu.make_async_copy(v_hbm, vp.at[:, inner, :], load_sem.at[1]),
        pltpu.make_async_copy(dp_hbm, dpp.at[inner, :], load_sem.at[2]),
        pltpu.make_async_copy(wm_hbm, wmb, load_sem.at[3]),
        pltpu.make_async_copy(
            tr_hbm.at[pl.ds(0, 2)], trp.at[pl.ds(0, 2), :, inner, :], load_sem.at[4]
        ),
        pltpu.make_async_copy(
            tr_hbm.at[pl.ds(2, nt - 2)], trp.at[pl.ds(2, nt - 2), :, inner, :], load_sem.at[9]
        ),
        pltpu.make_async_copy(sf_hbm, sfb, load_sem.at[5]),
        pltpu.make_async_copy(kin_hbm, kin, load_sem.at[6]),
        pltpu.make_async_copy(rc_hbm, rc, load_sem.at[7]),
        pltpu.make_async_copy(rl_hbm, rl, load_sem.at[8]),
    ]
    for load in loads:
        load.start()

    neighbours = [
        (None, {"grp": first}),
        (None, {"grp": second}),
        (None, {"grp": third}),
        (gy > 0, {"ty": gy - 1}),
        (gy < n_ty - 1, {"ty": gy + 1}),
        (gt > 0, {"tx": gt - 1}),
        (gt < n_tx - 1, {"tx": gt + 1}),
    ]
    barrier = pltpu.get_barrier_semaphore()
    for there, device in neighbours:
        if there is None:
            pl.semaphore_signal(barrier, inc=1, device_id=device, device_id_type=MESH)
        else:

            @pl.when(there)
            def _(device=device):
                pl.semaphore_signal(barrier, inc=1, device_id=device, device_id_type=MESH)

    def remote(src, dst, ss, rs, device):
        return pltpu.make_async_remote_copy(
            src_ref=src, dst_ref=dst, send_sem=ss, recv_sem=rs, device_id=device, device_id_type=MESH
        )

    to_north = remote(ns_send.at[0], ns_recv.at[0], halo_ss.at[0], halo_rs.at[0], {"ty": gy + 1})
    to_south = remote(ns_send.at[1], ns_recv.at[1], halo_ss.at[1], halo_rs.at[1], {"ty": gy - 1})
    to_east = remote(ew_send.at[0], ew_recv.at[0], halo_ss.at[2], halo_rs.at[2], {"tx": gt + 1})
    to_west = remote(ew_send.at[1], ew_recv.at[1], halo_ss.at[3], halo_rs.at[3], {"tx": gt - 1})
    halo_sends = [
        (gy < n_ty - 1, to_north),
        (gy > 0, to_south),
        (gt < n_tx - 1, to_east),
        (gt > 0, to_west),
    ]
    halo_recvs = [
        (gy > 0, to_north),
        (gy < n_ty - 1, to_south),
        (gt > 0, to_east),
        (gt < n_tx - 1, to_west),
    ]
    sd_first = remote(sdb, sdr.at[0], red_ss.at[0], red_rs.at[0], {"grp": first})
    sd_second = remote(sdp, sdr.at[1], red_ss.at[1], red_rs.at[1], {"grp": second})
    flows = pl.ds(4 * nt, 8)
    flow_copies = [
        remote(xt.at[flows, :], er.at[i], e_ss.at[i], e_rs.at[i], {"grp": device})
        for i, device in enumerate((first, second, third))
    ]
    low, high = pl.ds(0, 2 * nt), pl.ds(2 * nt, 2 * nt)
    x_up = remote(xt.at[low, :], xr.at[high, :], x_ss.at[0], x_rs.at[0], {"grp": g - 1})
    x_down = remote(xt.at[high, :], xr.at[low, :], x_ss.at[1], x_rs.at[1], {"grp": g + 1})
    p2_west = remote(
        c2t.at[pl.ds(0, 8), :], e2.at[pl.ds(0, 8), :], p2_ss.at[0], p2_rs.at[0], {"tx": gt - 1}
    )
    p2_south = remote(r2, n2, p2_ss.at[1], p2_rs.at[1], {"ty": gy - 1})

    n_pairs = blocks // 2 - 1

    def blocks_of(i):
        return pl.ds(2 * i + 1, 2)

    def bulk_up(span, sem):
        return remote(adv.at[0, span], gb.at[span], bulk_ss.at[0, sem], bulk_rs.at[0, sem], {"grp": g - 1})

    def bulk_down(span, sem):
        return remote(adv.at[1, span], ga.at[span], bulk_ss.at[1, sem], bulk_rs.at[1, sem], {"grp": g + 1})

    def send_bulk(span, sem):
        @pl.when(up_there)
        def _():
            bulk_up(span, sem).start()

        @pl.when(down_there)
        def _():
            bulk_down(span, sem).start()

    def await_bulk(span, sem):
        @pl.when(up_there)
        def _():
            bulk_down(span, sem).wait_recv()

        @pl.when(down_there)
        def _():
            bulk_up(span, sem).wait_recv()

    def await_sent(span, sem):
        @pl.when(up_there)
        def _():
            bulk_up(span, sem).wait_send()

        @pl.when(down_there)
        def _():
            bulk_down(span, sem).wait_send()

    def single(i):
        return pl.ds(i * (blocks - 1), 1), n_pairs + i

    def couple(i):
        return blocks_of(i), i

    def loop(start, stop, body):
        lax.fori_loop(start, stop, lambda i, c: (body(i), c)[1], 0)

    zero = jnp.zeros((8, lanes), f32)
    zero_t = jnp.zeros((TALL, lanes), f32)
    talls = rows // TALL

    def clear(ref):
        def one(i):
            ref[blk(i), :] = zero

        loop(0, ref.shape[0] // 8, one)

    def clear_ghost(ref):
        def one(i):
            for n in range(nt):
                ref[i, n] = zero

        loop(0, blocks, one)

    @pl.when(jnp.logical_not(up_there))
    def _():
        clear_ghost(ga)
        clear(xr.at[low, :])

    @pl.when(jnp.logical_not(down_there))
    def _():
        clear_ghost(gb)
        clear(xr.at[high, :])

    clear(xr.at[pl.ds(4 * nt + 8, lanes - 4 * nt - 8), :])
    clear(mt.at[pl.ds(80, lanes - 80), :])
    clear(e2.at[pl.ds(8, lanes - 8), :])

    for slot, (there, _) in enumerate(halo_recvs):

        @pl.when(jnp.logical_not(there))
        def _(slot=slot):
            clear(ns_recv.at[slot] if slot < 2 else ew_recv.at[slot - 2])

    @pl.when(gt == n_tx - 1)
    def _():
        e2[pl.ds(0, 8), :] = zero

    @pl.when(gy == n_ty - 1)
    def _():
        n2[...] = zero

    for load in loads[:4]:
        load.wait()
    for edge in (0, PAD + rows):
        dpp[pl.ds(edge, 8), :] = zero
        wp[pl.ds(edge, 8), :] = zero
    for l in range(2):
        gp[l, pl.ds(0, 8), :] = zero

    def wetness(i):
        wp[mid(i, TALL), :] = wmb[tall(i), :].astype(f32)

    loop(0, talls, wetness)

    def north_face(i, n):
        d, w = dpp[mid(i, n), :], wp[mid(i, n), :]
        depth_n = (0.5 / levels) * (d + dpp[north(i, n), :]) * (w * wp[north(i, n), :])
        for l in range(2):
            gp[l, mid(i, n), :] = vp[l, mid(i, n), :] * depth_n

    def faces(i):
        d, w = dpp[mid(i, TALL), :], wp[mid(i, TALL), :]
        depth_e = (0.5 / levels) * (d + roll(d, -1)) * (w * roll(w, -1))
        depth_e = jnp.where(at_east, 0.0, depth_e)
        for l in range(2):
            fb[l, tall(i), :] = up[l, mid(i, TALL), :] * depth_e
        north_face(i, TALL)

    loop(0, talls, faces)

    def divergence(i):
        east = fb[0, tall(i), :] + fb[1, tall(i), :]
        in_n = gp[0, mid(i, TALL), :] + gp[1, mid(i, TALL), :]
        in_s = gp[0, south(i, TALL), :] + gp[1, south(i, TALL), :]
        sdb[1, tall(i), :] = (east - roll(east, 1)) + (in_n - in_s)

    loop(0, talls, divergence)
    loads[4].wait()

    def density(i):
        salt = trp[0, 0, mid(i, TALL), :] + trp[0, 1, mid(i, TALL), :]
        heat = trp[1, 0, mid(i, TALL), :] + trp[1, 1, mid(i, TALL), :]
        sdb[0, tall(i), :] = haline_coef * salt - thermal_coef * heat

    loop(0, talls, density)

    peers = sum(1 if there is None else there.astype(jnp.int32) for there, _ in neighbours)
    pl.semaphore_wait(barrier, peers)
    sd_first.start()

    loads[5].wait()

    def edges(i):
        packed = zero_t
        fields = [trp.at[n, l] for l in range(2) for n in range(nt)]
        fields += [up.at[0], up.at[1], vp.at[0], vp.at[1], dpp, wp]
        for f, field in enumerate(fields):
            packed = jnp.where(pair == f, roll(field[mid(i, TALL), :], 2 * f + 1), packed)
        q[tall(i), :] = packed

    loop(0, talls, edges)
    qt[...] = jnp.transpose(q[...])
    for side in range(2):
        ew_send[side] = qt[pl.ds(side, 40, stride=2), :]

    padded = [trp.at[n, l] for l in range(2) for n in range(nt)]
    padded += [up.at[0], up.at[1], vp.at[0], vp.at[1], dpp, wp]
    for slot in range(2):
        ns_send[slot, pl.ds(32, 8), :] = zero
    for f, ref in enumerate(padded):
        ns_send[0, pl.ds(f, 1), :] = ref[pl.ds(PAD + rows - 1, 1), :]
        ns_send[1, pl.ds(f, 1), :] = ref[pl.ds(PAD, 1), :]

    for there, copy in reversed(halo_sends):

        @pl.when(there)
        def _(copy=copy):
            copy.start()

    def advect(r):
        d = dpp[mid(r), :]
        scale = (advect_rate * levels) / d
        for l in range(2):
            fe, gn, gs = fb[l, blk(r), :], gp[l, mid(r), :], gp[l, south(r), :]
            fw = roll(fe, 1)
            out = (jnp.maximum(fe, 0.0) - jnp.minimum(fw, 0.0)) + (
                jnp.maximum(gn, 0.0) - jnp.minimum(gs, 0.0)
            )
            own = 1.0 - scale * out
            from_e, from_w = -scale * jnp.minimum(fe, 0.0), scale * jnp.maximum(fw, 0.0)
            from_n, from_s = -scale * jnp.minimum(gn, 0.0), scale * jnp.maximum(gs, 0.0)
            for n in range(nt):
                c = trp[n, l, mid(r), :]
                adv[l, r, n] = (
                    (own * c + from_e * roll(c, -1))
                    + (from_w * roll(c, 1) + from_n * trp[n, l, north(r), :])
                    + from_s * trp[n, l, south(r), :]
                )

    def advect_and_send(i):
        advect(2 * i + 1)
        advect(2 * i + 2)

        @pl.when(jnp.logical_and(i > 0, i <= BULK_FIRST))
        def _():
            send_bulk(*couple(i - 1))

    loop(0, n_pairs, advect_and_send)

    sd_first.wait_recv()

    def pair_sums(i):
        for k in range(2):
            sdp[k, tall(i), :] = sdb[k, tall(i), :] + sdr[0, k, tall(i), :]

    loop(0, talls, pair_sums)

    for load in loads[6:]:
        load.wait()

    def spread(n):
        for m in range(nt):
            kb[n, m] = jnp.full((8, lanes), kin[n, m], f32)

    loop(0, nt, spread)
    sd_second.start()

    for there, copy in halo_recvs:

        @pl.when(there)
        def _(copy=copy):
            copy.wait_recv()

    for f, ref in enumerate(padded):
        ref[pl.ds(PAD - 1, 1), :] = ns_recv[0, pl.ds(f, 1), :]
        ref[pl.ds(PAD + rows, 1), :] = ns_recv[1, pl.ds(f, 1), :]
    d_south, w_south = dpp[pl.ds(PAD - 1, 1), :], wp[pl.ds(PAD - 1, 1), :]
    d_row, w_row = dpp[pl.ds(PAD, 1), :], wp[pl.ds(PAD, 1), :]
    depth_s = (0.5 / levels) * (d_south + d_row) * (w_south * w_row)
    for l in range(2):
        gp[l, pl.ds(PAD - 1, 1), :] = vp[l, pl.ds(PAD - 1, 1), :] * depth_s
    north_face(blocks - 1, 8)
    for side in range(2):
        mt[pl.ds(side, 40, stride=2), :] = ew_recv[1 - side]
    mb[...] = jnp.transpose(mt[...])

    def rim(i):
        m = mb[tall(i), :]
        d, w = dpp[mid(i, TALL), :], wp[mid(i, TALL), :]
        scale = (advect_rate * levels) / d
        depth_f = (0.5 / levels) * (d + unpacked(m, f_d)) * (w * unpacked(m, f_w))
        total = zero_t
        parts = []
        for l in range(2):
            flow = jnp.where(at_west, unpacked(m, n_uv + l), up[l, mid(i, TALL), :])
            flux = jnp.where(at_edge, flow * depth_f, 0.0)
            total = total + jnp.where(at_east, flux, -flux)
            z = scale * flux
            z_e = jnp.broadcast_to(z[:, lanes - 1 : lanes], (TALL, lanes))
            z_w = jnp.broadcast_to(z[:, 0:1], (TALL, lanes))
            parts.append(jnp.where(even, -z_e, z_w))
        zz = jnp.where(lane_t < 2 * nt, parts[0], parts[1])
        x = jnp.minimum(zz, 0.0) * q[tall(i), :] + jnp.maximum(zz, 0.0) * m
        xb[tall(i), :] = jnp.where(pair == n_uv, roll(total, 2 * n_uv + 1), x)

    loop(0, talls, rim)
    xt[...] = jnp.transpose(xb[...])
    xt[pl.ds(4 * nt + 2, 1), :] = gp[0, pl.ds(PAD + rows - 1, 1), :] + gp[1, pl.ds(PAD + rows - 1, 1), :]
    xt[pl.ds(4 * nt + 3, 1), :] = -(gp[0, pl.ds(PAD - 1, 1), :] + gp[1, pl.ds(PAD - 1, 1), :])
    advect(0)
    for copy in reversed(flow_copies):
        copy.start()

    @pl.when(up_there)
    def _():
        x_up.start()

    @pl.when(down_there)
    def _():
        x_down.start()

    loop(BULK_FIRST, n_pairs, lambda i: send_bulk(*couple(i)))
    advect(blocks - 1)

    sd_second.wait_recv()
    over_first = (lax.rem(g, 2) == 1).astype(f32)
    over_second = (g >= 2).astype(f32)
    press = baroclinic_rate / levels

    def pressure(i):
        over = over_first * sdr[0, 0, tall(i), :] + over_second * sdr[1, 0, tall(i), :]
        dens = [
            haline_coef * trp[0, l, mid(i, TALL), :] - thermal_coef * trp[1, l, mid(i, TALL), :]
            for l in range(2)
        ]
        d = press * dpp[mid(i, TALL), :]
        pp[0, tall(i), :] = d * (over + 0.5 * dens[0])
        pp[1, tall(i), :] = d * (over + dens[0] + 0.5 * dens[1])

    loop(0, talls, pressure)
    loop(0, 2, lambda i: send_bulk(*single(i)))

    @pl.when(up_there)
    def _():
        x_down.wait_recv()

    @pl.when(down_there)
    def _():
        x_up.wait_recv()

    for copy in flow_copies:
        copy.wait_recv()
    flow_sum = (xt[flows, :] + er[0]) + (er[1] + er[2])
    xr[flows, :] = flow_sum
    yb[...] = jnp.transpose(xr[...])
    mix_up = jnp.where(up_there, mixing_rate, 0.0).astype(f32)
    mix_down = jnp.where(down_there, mixing_rate, 0.0).astype(f32)
    own_up = (1.0 - mixing_rate) - mix_up
    own_down = (1.0 - mixing_rate) - mix_down

    flow_n, flow_s = flow_sum[2:3, :], flow_sum[3:4, :]

    def surface(i):
        row = i * TALL + sub_t
        across = jnp.where(at_edge, unpacked(yb[tall(i), :], n_uv), 0.0)
        across = across + jnp.where(row == rows - 1, flow_n, jnp.where(row == 0, flow_s, 0.0))
        total = (sdp[1, tall(i), :] + sdr[1, 1, tall(i), :]) + across
        ns = sfb[tall(i), :] - eta_rate * wp[mid(i, TALL), :] * total
        out_s[tall(i), :] = ns
        nsp[tall(i), :] = ns
        p0, p1 = pp[0, tall(i), :], pp[1, tall(i), :]
        c2[tall(i), :] = jnp.where(
            lane_t == 0, ns, jnp.where(lane_t == 1, roll(p0, 1), jnp.where(lane_t == 2, roll(p1, 2), 0.0))
        )

    loop(0, talls, surface)
    r2[...] = zero
    r2[pl.ds(0, 1), :] = nsp[pl.ds(0, 1), :]
    for l in range(2):
        r2[pl.ds(1 + l, 1), :] = pp[l, pl.ds(0, 1), :]
    c2t[...] = jnp.transpose(c2[...])

    @pl.when(gt > 0)
    def _():
        p2_west.start()

    @pl.when(gy > 0)
    def _():
        p2_south.start()

    def blend_edges(i):
        x = xb[tall(i), :]
        is_top = lane_t < 2 * nt
        other = jnp.where(is_top, roll(x, -2 * nt), roll(x, 2 * nt))
        bx[tall(i), :] = (
            jnp.where(is_top, own_up, own_down) * x
            + mixing_rate * other
            + jnp.where(is_top, mix_up, mix_down) * yb[tall(i), :]
        )

    loop(0, talls, blend_edges)

    is_top_level = (g == 0).astype(f32)

    def finish(r):
        w = wp[mid(r), :]
        edge = bx[blk(r), :]
        updated = [[], []]
        for n in range(nt):
            a0, a1 = adv[0, r, n], adv[1, r, n]
            e0 = jnp.where(short_edge, unpacked(edge, n), 0.0)
            e1 = jnp.where(short_edge, unpacked(edge, nt + n), 0.0)
            b0 = (own_up * a0 + mixing_rate * a1) + (mix_up * ga[r, n] + e0)
            b1 = (own_down * a1 + mixing_rate * a0) + (mix_down * gb[r, n] + e1)
            for l, b in enumerate((b0, b1)):
                c = trp[n, l, mid(r), :]
                updated[l].append(c + w * (b - c))
        warm = [w * jnp.exp(warming_rate * updated[l][1]) for l in range(2)]
        cell = (r * 8 + sub) * lanes + lane
        top = is_top_level * w
        hits = [jnp.where(cell == rc[i], top, 0.0) for i in range(rc.shape[0])]
        for n in range(nt):
            k = kb[n, 0]
            react = [k * updated[l][0] for l in range(2)]
            for m in range(1, nt):
                k = kb[n, m]
                react = [react[l] + k * updated[l][m] for l in range(2)]
            source = hits[0] * rl[0, n]
            for i in range(1, rc.shape[0]):
                source = source + hits[i] * rl[i, n]
            out_tr[n, 0, blk(r), :] = updated[0][n] + (warm[0] * react[0] + source)
            out_tr[n, 1, blk(r), :] = updated[1][n] + warm[1] * react[1]

    def finish_couple(i):
        await_bulk(*couple(i))
        loop(2 * i + 1, 2 * i + 3, finish)

    def finish_single(i):
        await_bulk(*single(i))
        finish(i * (blocks - 1))

    loop(0, VELOCITIES_AFTER, finish_couple)

    @pl.when(gt < n_tx - 1)
    def _():
        p2_west.wait_recv()

    @pl.when(gy < n_ty - 1)
    def _():
        p2_south.wait_recv()

    t2[...] = jnp.transpose(e2[...])
    nsp[pl.ds(rows, 1), :] = n2[pl.ds(0, 1), :]
    for l in range(2):
        pp[l, pl.ds(rows, 1), :] = n2[pl.ds(1 + l, 1), :]
    friction = jnp.where(g == n_grp - 1, friction_rate, 0.0).astype(f32)

    def velocities(i):
        m = mb[tall(i), :]
        t = t2[tall(i), :]
        w = wp[mid(i, TALL), :]
        open_e = w * jnp.where(at_east, unpacked(m, f_w), roll(w, -1))
        open_n = w * wp[north(i, TALL), :]
        above = pl.ds(i * TALL + 1, TALL)
        ns = nsp[tall(i), :]
        slope_e = jnp.where(at_east, roll(t, -1), roll(ns, -1)) - ns
        slope_n = nsp[above, :] - ns
        for l in range(2):
            p = pp[l, tall(i), :]
            push_e = jnp.where(at_east, roll(t, -2 - l), roll(p, -1)) - p
            push_n = pp[l, above, :] - p
            for ref, out, field, opened, slope, push in (
                (up, out_u, n_uv + l, open_e, slope_e, push_e),
                (vp, out_v, n_uv + 2 + l, open_n, slope_n, push_n),
            ):
                x = ref[l, mid(i, TALL), :]
                beside = unpacked(m, field)
                lap = (
                    (ref[l, north(i, TALL), :] + ref[l, south(i, TALL), :])
                    + (jnp.where(at_east, beside, roll(x, -1)) + jnp.where(at_west, beside, roll(x, 1)))
                    - 4.0 * x
                )
                new = x - gravity_rate * slope - push + viscous_rate * lap
                if l == 1:
                    new = new - friction * x
                out[l, tall(i), :] = opened * new

    loop(0, talls, velocities)
    loop(VELOCITIES_AFTER, n_pairs, finish_couple)
    loop(0, 2, finish_single)

    for copy in [sd_first, sd_second, *flow_copies]:
        copy.wait_send()
    for there, copy in halo_sends + [
        (up_there, x_up),
        (down_there, x_down),
        (gt > 0, p2_west),
        (gy > 0, p2_south),
    ]:

        @pl.when(there)
        def _(copy=copy):
            copy.wait_send()

    loop(0, n_pairs, lambda i: await_sent(*couple(i)))
    loop(0, 2, lambda i: await_sent(*single(i)))


def put_kernel(*refs):
    sources, targets, sem = refs[:4], refs[4:8], refs[8]
    puts = [pltpu.make_async_copy(a, b, sem.at[i]) for i, (a, b) in enumerate(zip(sources, targets))]
    for put in puts:
        put.start()
    for put in puts:
        put.wait()


def shards(tracers, east_velocity, north_velocity, surface, depth, wet_mask, river_cells, river_loads, kinetics):
    nt, own, rows, lanes = tracers.shape
    levels = own * lax.axis_size("grp")
    blocks = rows // 8
    tall = rows + 2 * PAD
    tile = pltpu.VMEM((rows, lanes), f32)
    twice = pltpu.VMEM((2, rows, lanes), f32)
    edges = pltpu.VMEM((2, 40, lanes), f32)
    dma = pltpu.SemaphoreType.DMA
    scratch = [
        pltpu.VMEM((nt, 2, tall, lanes), f32),
        pltpu.VMEM((2, tall, lanes), f32),
        pltpu.VMEM((2, tall, lanes), f32),
        tile,
        pltpu.VMEM((tall, lanes), f32),
        pltpu.VMEM((rows, lanes), jnp.int32),
        pltpu.VMEM((tall, lanes), f32),
        pltpu.VMEM((nt, nt, 8, lanes), f32),
        twice,
        pltpu.VMEM((2, tall, lanes), f32),
        twice,
        twice,
        pltpu.VMEM((2, 2, rows, lanes), f32),
        edges,
        edges,
        tile,
        tile,
        edges,
        edges,
        tile,
        tile,
        tile,
        tile,
        tile,
        pltpu.VMEM((3, 8, lanes), f32),
        tile,
        tile,
        pltpu.VMEM((2, blocks, nt, 8, lanes), f32),
        pltpu.VMEM((blocks, nt, 8, lanes), f32),
        pltpu.VMEM((blocks, nt, 8, lanes), f32),
        pltpu.VMEM((rows + 8, lanes), f32),
        pltpu.VMEM((2, rows + 8, lanes), f32),
        tile,
        tile,
        tile,
        tile,
        pltpu.VMEM((8, lanes), f32),
        pltpu.VMEM((8, lanes), f32),
        pltpu.SMEM(river_cells.shape, jnp.int32),
        pltpu.SMEM(river_loads.shape, f32),
        pltpu.SMEM((nt, nt), f32),
        dma((10,)),
        dma((4,)),
        dma((4,)),
        dma((2,)),
        dma((2,)),
        dma((3,)),
        dma((3,)),
        dma((2,)),
        dma((2,)),
        dma((2,)),
        dma((2,)),
        dma((2, blocks)),
        dma((2, blocks)),
    ]
    anywhere = pl.BlockSpec(memory_space=pltpu.HBM)
    vmem = pl.BlockSpec(memory_space=pltpu.VMEM)
    outs = (
        jax.ShapeDtypeStruct(tracers.shape, f32),
        jax.ShapeDtypeStruct(east_velocity.shape, f32),
        jax.ShapeDtypeStruct(north_velocity.shape, f32),
        jax.ShapeDtypeStruct(surface.shape, f32),
    )
    fields = [
        pltpu.with_memory_space_constraint(x, pltpu.HBM)
        for x in (
            tracers, east_velocity, north_velocity, surface, depth, wet_mask,
            river_cells, river_loads, kinetics,
        )
    ]
    results = pl.pallas_call(
        functools.partial(step_kernel, levels),
        out_shape=outs,
        in_specs=[anywhere] * 9,
        out_specs=(vmem,) * 4,
        scratch_shapes=scratch,
        compiler_params=pltpu.CompilerParams(
            collective_id=0, has_side_effects=True, vmem_limit_bytes=32 * 1024 * 1024
        ),
        name="estuary_step",
    )(*fields)
    return pl.pallas_call(
        put_kernel,
        out_shape=outs,
        in_specs=[pl.BlockSpec(memory_space=pl.ANY)] * 4,
        out_specs=(pl.BlockSpec(memory_space=pl.ANY),) * 4,
        scratch_shapes=[dma((4,))],
        compiler_params=pltpu.CompilerParams(vmem_limit_bytes=1024 * 1024),
        name="put",
    )(*results)


def solution(mesh):
    return jax.shard_map(
        shards,
        mesh=mesh,
        in_specs=(
            P(None, "grp", "ty", "tx"),
            P("grp", "ty", "tx"),
            P("grp", "ty", "tx"),
            P("ty", "tx"),
            P("ty", "tx"),
            P("ty", "tx"),
            P(("ty", "tx")),
            P(("ty", "tx"), None),
            P(),
        ),
        out_specs=(
            P(None, "grp", "ty", "tx"),
            P("grp", "ty", "tx"),
            P("grp", "ty", "tx"),
            P("ty", "tx"),
        ),
        check_vma=False,
    )
```

```python
import functools

import jax
import jax.numpy as jnp
from jax import lax
from jax.experimental import pallas as pl
from jax.experimental.pallas import tpu as pltpu
from jax.sharding import PartitionSpec as P

f32 = jnp.float32
MESH = pl.DeviceIdType.MESH

eta_rate = 0.25
gravity_rate = 0.25
baroclinic_rate = 0.4
viscous_rate = 0.1
friction_rate = 0.3
advect_rate = 0.3
mixing_rate = 0.2
haline_coef = 0.8
thermal_coef = 0.2
warming_rate = 0.46

PAD = 8
TALL = 32
BULK_FIRST = 3
BULK_MIDDLE = 4
VELOCITIES_AFTER = 7


def step_kernel(
    levels,
    tr_hbm, u_hbm, v_hbm, sf_hbm, dp_hbm, wm_hbm, rc_hbm, rl_hbm, kin_hbm,
    out_tr, out_u, out_v, out_s,
    trp, up, vp, sfb, dpp, wmb, wp, kb,
    fb, gp, sdb, d_in, s_in, d_half, s_half, s_other, d_all, s_over,
    ns_send, ns_recv, q, qt, ew_send, ew_recv, mt, mb,
    xb, xt, xr, er, yb, bx, adv, ga, gb,
    nsp, pp, c2, c2t, e2, t2, r2, n2,
    rc, rl, kin, load_sem, halo_ss, halo_rs, red_ss, red_rs, e_ss, e_rs, x_ss, x_rs, p2_ss, p2_rs, bulk_ss, bulk_rs,
):
    g, gy, gt = lax.axis_index("grp"), lax.axis_index("ty"), lax.axis_index("tx")
    n_grp, n_ty, n_tx = lax.axis_size("grp"), lax.axis_size("ty"), lax.axis_size("tx")
    nt = tr_hbm.shape[0]
    rows, lanes = sfb.shape
    blocks = rows // 8
    n_uv = 2 * nt
    f_d, f_w = n_uv + 4, n_uv + 5

    up_there, down_there = g > 0, g < n_grp - 1
    first = g + 1 - 2 * lax.rem(g, 2)
    second = n_grp - 1 - g
    third = lax.rem(g + n_grp // 2, n_grp)

    lane = lax.broadcasted_iota(jnp.int32, (8, lanes), 1)
    sub = lax.broadcasted_iota(jnp.int32, (8, lanes), 0)
    short_edge = jnp.logical_or(lane == lanes - 1, lane == 0)
    lane_t = lax.broadcasted_iota(jnp.int32, (TALL, lanes), 1)
    sub_t = lax.broadcasted_iota(jnp.int32, (TALL, lanes), 0)
    pair = lane_t // 2
    even = lax.rem(lane_t, 2) == 0
    at_east, at_west = lane_t == lanes - 1, lane_t == 0
    at_edge = jnp.logical_or(at_east, at_west)

    def roll(x, shift):
        shift = shift % lanes
        return x if shift == 0 else pltpu.roll(x, shift, 1)

    def unpacked(tile, field):
        return roll(tile, lanes - 1 - 2 * field)

    def blk(r):
        return pl.ds(pl.multiple_of(r * 8, 8), 8)

    def part(which, i):
        return pl.ds(pl.multiple_of(which * (rows // 2) + i * TALL, TALL), TALL)

    def tall(i):
        return pl.ds(pl.multiple_of(i * TALL, TALL), TALL)

    def mid(r, n=8):
        return pl.ds(pl.multiple_of(r * n + PAD, 8), n)

    def south(r, n=8):
        return pl.ds(r * n + (PAD - 1), n)

    def north(r, n=8):
        return pl.ds(r * n + (PAD + 1), n)

    neighbours = [
        (gt > 0, {"tx": gt - 1}),
        (gt < n_tx - 1, {"tx": gt + 1}),
        (None, {"grp": first}),
        (None, {"grp": second}),
        (None, {"grp": third}),
        (gy > 0, {"ty": gy - 1}),
        (gy < n_ty - 1, {"ty": gy + 1}),
    ]
    barrier = pltpu.get_barrier_semaphore()
    for there, device in neighbours:
        if there is None:
            pl.semaphore_signal(barrier, inc=1, device_id=device, device_id_type=MESH)
        else:

            @pl.when(there)
            def _(device=device):
                pl.semaphore_signal(barrier, inc=1, device_id=device, device_id_type=MESH)

    inner = pl.ds(PAD, rows)
    loads = [
        pltpu.make_async_copy(u_hbm, up.at[:, inner, :], load_sem.at[0]),
        pltpu.make_async_copy(v_hbm, vp.at[:, inner, :], load_sem.at[1]),
        pltpu.make_async_copy(dp_hbm, dpp.at[inner, :], load_sem.at[2]),
        pltpu.make_async_copy(wm_hbm, wmb, load_sem.at[3]),
        pltpu.make_async_copy(
            tr_hbm.at[pl.ds(0, 2)], trp.at[pl.ds(0, 2), :, inner, :], load_sem.at[4]
        ),
        pltpu.make_async_copy(
            tr_hbm.at[pl.ds(2, nt - 2)], trp.at[pl.ds(2, nt - 2), :, inner, :], load_sem.at[9]
        ),
        pltpu.make_async_copy(sf_hbm, sfb, load_sem.at[5]),
        pltpu.make_async_copy(kin_hbm, kin, load_sem.at[6]),
        pltpu.make_async_copy(rc_hbm, rc, load_sem.at[7]),
        pltpu.make_async_copy(rl_hbm, rl, load_sem.at[8]),
    ]
    for load in loads:
        load.start()

    def remote(src, dst, ss, rs, device):
        return pltpu.make_async_remote_copy(
            src_ref=src, dst_ref=dst, send_sem=ss, recv_sem=rs, device_id=device, device_id_type=MESH
        )

    to_north = remote(ns_send.at[0], ns_recv.at[0], halo_ss.at[0], halo_rs.at[0], {"ty": gy + 1})
    to_south = remote(ns_send.at[1], ns_recv.at[1], halo_ss.at[1], halo_rs.at[1], {"ty": gy - 1})
    to_east = remote(ew_send.at[0], ew_recv.at[0], halo_ss.at[2], halo_rs.at[2], {"tx": gt + 1})
    to_west = remote(ew_send.at[1], ew_recv.at[1], halo_ss.at[3], halo_rs.at[3], {"tx": gt - 1})
    halo_sends = [
        (gy < n_ty - 1, to_north),
        (gy > 0, to_south),
        (gt < n_tx - 1, to_east),
        (gt > 0, to_west),
    ]
    halo_recvs = [
        (gy > 0, to_north),
        (gy < n_ty - 1, to_south),
        (gt > 0, to_east),
        (gt < n_tx - 1, to_west),
    ]
    half = rows // 2
    d_half_at, s_half_at = lax.rem((g + 1) // 2, 2), g // 2

    def half_at(i):
        return pl.ds(pl.multiple_of(i * half, half), half)

    d_mine, d_other = half_at(d_half_at), half_at(1 - d_half_at)
    s_mine, s_theirs = half_at(s_half_at), half_at(1 - s_half_at)

    def reduction(i, src, dst, device):
        return remote(src, dst, red_ss.at[i], red_rs.at[i], {"grp": device})

    d_copies = [
        reduction(0, sdb.at[1, d_other, :], d_in.at[0], first),
        reduction(1, d_half, d_in.at[1], second),
        reduction(2, d_all.at[d_mine, :], d_all.at[d_mine, :], first),
    ]
    s_copies = [
        reduction(3, sdb.at[0, s_theirs, :], s_in.at[0], second),
        reduction(4, s_half, s_in.at[1], first),
        reduction(5, s_other, s_over.at[s_mine, :], second),
    ]
    d_last = reduction(2, d_all.at[d_other, :], d_all.at[d_other, :], first)
    s_last = reduction(5, s_other, s_over.at[s_theirs, :], second)
    flows = pl.ds(4 * nt, 8)
    flow_copies = [
        remote(xt.at[flows, :], er.at[i], e_ss.at[i], e_rs.at[i], {"grp": device})
        for i, device in enumerate((first, second, third))
    ]
    low, high = pl.ds(0, 2 * nt), pl.ds(2 * nt, 2 * nt)
    x_up = remote(xt.at[low, :], xr.at[high, :], x_ss.at[0], x_rs.at[0], {"grp": g - 1})
    x_down = remote(xt.at[high, :], xr.at[low, :], x_ss.at[1], x_rs.at[1], {"grp": g + 1})
    p2_west = remote(
        c2t.at[pl.ds(0, 8), :], e2.at[pl.ds(0, 8), :], p2_ss.at[0], p2_rs.at[0], {"tx": gt - 1}
    )
    p2_south = remote(r2, n2, p2_ss.at[1], p2_rs.at[1], {"ty": gy - 1})

    n_pairs = blocks // 2 - 1

    def blocks_of(i):
        return pl.ds(2 * i + 1, 2)

    def bulk_up(span, sem):
        return remote(adv.at[0, span], gb.at[span], bulk_ss.at[0, sem], bulk_rs.at[0, sem], {"grp": g - 1})

    def bulk_down(span, sem):
        return remote(adv.at[1, span], ga.at[span], bulk_ss.at[1, sem], bulk_rs.at[1, sem], {"grp": g + 1})

    def send_bulk(span, sem):
        @pl.when(up_there)
        def _():
            bulk_up(span, sem).start()

        @pl.when(down_there)
        def _():
            bulk_down(span, sem).start()

    def await_bulk(span, sem):
        @pl.when(up_there)
        def _():
            bulk_down(span, sem).wait_recv()

        @pl.when(down_there)
        def _():
            bulk_up(span, sem).wait_recv()

    def await_sent(span, sem):
        @pl.when(up_there)
        def _():
            bulk_up(span, sem).wait_send()

        @pl.when(down_there)
        def _():
            bulk_down(span, sem).wait_send()

    def single(i):
        return pl.ds(i * (blocks - 1), 1), n_pairs + i

    def couple(i):
        return blocks_of(i), i

    def loop(start, stop, body):
        lax.fori_loop(start, stop, lambda i, c: (body(i), c)[1], 0)

    zero = jnp.zeros((8, lanes), f32)
    zero_t = jnp.zeros((TALL, lanes), f32)
    talls = rows // TALL

    def clear(ref):
        def one(i):
            ref[blk(i), :] = zero

        loop(0, ref.shape[0] // 8, one)

    def clear_ghost(ref):
        def one(i):
            for n in range(nt):
                ref[i, n] = zero

        loop(0, blocks, one)

    @pl.when(jnp.logical_not(up_there))
    def _():
        clear_ghost(ga)
        clear(xr.at[low, :])

    @pl.when(jnp.logical_not(down_there))
    def _():
        clear_ghost(gb)
        clear(xr.at[high, :])

    clear(xr.at[pl.ds(4 * nt + 8, lanes - 4 * nt - 8), :])
    clear(mt.at[pl.ds(80, lanes - 80), :])
    clear(e2.at[pl.ds(8, lanes - 8), :])

    for slot, (there, _) in enumerate(halo_recvs):

        @pl.when(jnp.logical_not(there))
        def _(slot=slot):
            clear(ns_recv.at[slot] if slot < 2 else ew_recv.at[slot - 2])

    @pl.when(gt == n_tx - 1)
    def _():
        e2[pl.ds(0, 8), :] = zero

    @pl.when(gy == n_ty - 1)
    def _():
        n2[...] = zero

    for load in loads[:4]:
        load.wait()
    for edge in (0, PAD + rows):
        dpp[pl.ds(edge, 8), :] = zero
        wp[pl.ds(edge, 8), :] = zero
    for l in range(2):
        gp[l, pl.ds(0, 8), :] = zero

    def wetness(i):
        wp[mid(i, TALL), :] = wmb[tall(i), :].astype(f32)

    loop(0, talls, wetness)

    def north_face(i, n):
        d, w = dpp[mid(i, n), :], wp[mid(i, n), :]
        depth_n = (0.5 / levels) * (d + dpp[north(i, n), :]) * (w * wp[north(i, n), :])
        for l in range(2):
            gp[l, mid(i, n), :] = vp[l, mid(i, n), :] * depth_n

    def faces(i):
        d, w = dpp[mid(i, TALL), :], wp[mid(i, TALL), :]
        depth_e = (0.5 / levels) * (d + roll(d, -1)) * (w * roll(w, -1))
        depth_e = jnp.where(at_east, 0.0, depth_e)
        for l in range(2):
            fb[l, tall(i), :] = up[l, mid(i, TALL), :] * depth_e
        north_face(i, TALL)

    loop(0, talls, faces)

    def divergence(i):
        east = fb[0, tall(i), :] + fb[1, tall(i), :]
        in_n = gp[0, mid(i, TALL), :] + gp[1, mid(i, TALL), :]
        in_s = gp[0, south(i, TALL), :] + gp[1, south(i, TALL), :]
        sdb[1, tall(i), :] = (east - roll(east, 1)) + (in_n - in_s)

    loop(0, talls, divergence)
    loads[4].wait()

    def density(i):
        salt = trp[0, 0, mid(i, TALL), :] + trp[0, 1, mid(i, TALL), :]
        heat = trp[1, 0, mid(i, TALL), :] + trp[1, 1, mid(i, TALL), :]
        sdb[0, tall(i), :] = haline_coef * salt - thermal_coef * heat

    loop(0, talls, density)

    def advect(r):
        d = dpp[mid(r), :]
        scale = (advect_rate * levels) / d
        for l in range(2):
            fe, gn, gs = fb[l, blk(r), :], gp[l, mid(r), :], gp[l, south(r), :]
            fw = roll(fe, 1)
            out = (jnp.maximum(fe, 0.0) - jnp.minimum(fw, 0.0)) + (
                jnp.maximum(gn, 0.0) - jnp.minimum(gs, 0.0)
            )
            own = 1.0 - scale * out
            from_e, from_w = -scale * jnp.minimum(fe, 0.0), scale * jnp.maximum(fw, 0.0)
            from_n, from_s = -scale * jnp.minimum(gn, 0.0), scale * jnp.maximum(gs, 0.0)
            for n in range(nt):
                c = trp[n, l, mid(r), :]
                adv[l, r, n] = (
                    (own * c + from_e * roll(c, -1))
                    + (from_w * roll(c, 1) + from_n * trp[n, l, north(r), :])
                    + from_s * trp[n, l, south(r), :]
                )

    def advect_couple(i):
        advect(2 * i + 1)
        advect(2 * i + 2)

    loads[5].wait()
    loop(0, 1, advect_couple)

    peers = sum(1 if there is None else there.astype(jnp.int32) for there, _ in neighbours)
    pl.semaphore_wait(barrier, peers)
    d_copies[0].start()
    s_copies[0].start()

    send_bulk(*couple(0))


    def edges(i):
        packed = zero_t
        fields = [trp.at[n, l] for l in range(2) for n in range(nt)]
        fields += [up.at[0], up.at[1], vp.at[0], vp.at[1], dpp, wp]
        for f, field in enumerate(fields):
            packed = jnp.where(pair == f, roll(field[mid(i, TALL), :], 2 * f + 1), packed)
        q[tall(i), :] = packed

    loop(0, talls, edges)
    qt[...] = jnp.transpose(q[...])
    for side in range(2):
        ew_send[side] = qt[pl.ds(side, 40, stride=2), :]

    padded = [trp.at[n, l] for l in range(2) for n in range(nt)]
    padded += [up.at[0], up.at[1], vp.at[0], vp.at[1], dpp, wp]
    for slot in range(2):
        ns_send[slot, pl.ds(32, 8), :] = zero
    for f, ref in enumerate(padded):
        ns_send[0, pl.ds(f, 1), :] = ref[pl.ds(PAD + rows - 1, 1), :]
        ns_send[1, pl.ds(f, 1), :] = ref[pl.ds(PAD, 1), :]

    for there, copy in reversed(halo_sends):

        @pl.when(there)
        def _(copy=copy):
            copy.start()

    def advect_and_send(i):
        advect_couple(i)

        @pl.when(jnp.logical_and(i > 1, i <= BULK_FIRST))
        def _():
            send_bulk(*couple(i - 1))

    loop(1, n_pairs, advect_and_send)

    d_copies[0].wait_recv()
    s_copies[0].wait_recv()
    own_to_first = (g < n_grp - 1).astype(f32)
    second_to_first = (g > 0).astype(f32)

    def first_sums(i):
        d_half[tall(i), :] = sdb[1, part(d_half_at, i), :] + d_in[0, tall(i), :]
        s_half[tall(i), :] = (
            own_to_first * sdb[0, part(s_half_at, i), :] + second_to_first * s_in[0, tall(i), :]
        )

    loop(0, half // TALL, first_sums)

    for load in loads[6:]:
        load.wait()

    def spread(n):
        for m in range(nt):
            kb[n, m] = jnp.full((8, lanes), kin[n, m], f32)

    loop(0, nt, spread)
    d_copies[1].start()
    s_copies[1].start()
    loop(BULK_FIRST, BULK_MIDDLE, lambda i: send_bulk(*couple(i)))

    for there, copy in halo_recvs:

        @pl.when(there)
        def _(copy=copy):
            copy.wait_recv()

    for f, ref in enumerate(padded):
        ref[pl.ds(PAD - 1, 1), :] = ns_recv[0, pl.ds(f, 1), :]
        ref[pl.ds(PAD + rows, 1), :] = ns_recv[1, pl.ds(f, 1), :]
    d_south, w_south = dpp[pl.ds(PAD - 1, 1), :], wp[pl.ds(PAD - 1, 1), :]
    d_row, w_row = dpp[pl.ds(PAD, 1), :], wp[pl.ds(PAD, 1), :]
    depth_s = (0.5 / levels) * (d_south + d_row) * (w_south * w_row)
    for l in range(2):
        gp[l, pl.ds(PAD - 1, 1), :] = vp[l, pl.ds(PAD - 1, 1), :] * depth_s
    north_face(blocks - 1, 8)
    for side in range(2):
        mt[pl.ds(side, 40, stride=2), :] = ew_recv[1 - side]
    mb[...] = jnp.transpose(mt[...])

    def rim(i):
        m = mb[tall(i), :]
        d, w = dpp[mid(i, TALL), :], wp[mid(i, TALL), :]
        scale = (advect_rate * levels) / d
        depth_f = (0.5 / levels) * (d + unpacked(m, f_d)) * (w * unpacked(m, f_w))
        total = zero_t
        parts = []
        for l in range(2):
            flow = jnp.where(at_west, unpacked(m, n_uv + l), up[l, mid(i, TALL), :])
            flux = jnp.where(at_edge, flow * depth_f, 0.0)
            total = total + jnp.where(at_east, flux, -flux)
            z = scale * flux
            z_e = jnp.broadcast_to(z[:, lanes - 1 : lanes], (TALL, lanes))
            z_w = jnp.broadcast_to(z[:, 0:1], (TALL, lanes))
            parts.append(jnp.where(even, -z_e, z_w))
        zz = jnp.where(lane_t < 2 * nt, parts[0], parts[1])
        x = jnp.minimum(zz, 0.0) * q[tall(i), :] + jnp.maximum(zz, 0.0) * m
        xb[tall(i), :] = jnp.where(pair == n_uv, roll(total, 2 * n_uv + 1), x)

    loop(0, talls, rim)
    xt[...] = jnp.transpose(xb[...])
    xt[pl.ds(4 * nt + 2, 1), :] = gp[0, pl.ds(PAD + rows - 1, 1), :] + gp[1, pl.ds(PAD + rows - 1, 1), :]
    xt[pl.ds(4 * nt + 3, 1), :] = -(gp[0, pl.ds(PAD - 1, 1), :] + gp[1, pl.ds(PAD - 1, 1), :])
    d_copies[1].wait_recv()
    s_copies[1].wait_recv()
    above_1, above_2 = (g > 0).astype(f32), (g > 1).astype(f32)
    other_1, other_2 = (g < n_grp - 1).astype(f32), (g < 2).astype(f32)

    def second_sums(i):
        d_all[part(d_half_at, i), :] = d_half[tall(i), :] + d_in[1, tall(i), :]
        got = s_in[1, tall(i), :]
        s_over[part(s_half_at, i), :] = above_1 * got + above_2 * s_in[0, tall(i), :]
        s_other[tall(i), :] = other_1 * got + other_2 * sdb[0, part(s_half_at, i), :]

    loop(0, half // TALL, second_sums)
    advect(0)
    for copy in reversed(flow_copies):
        copy.start()
    d_copies[2].start()
    s_copies[2].start()

    @pl.when(up_there)
    def _():
        x_up.start()

    @pl.when(down_there)
    def _():
        x_down.start()

    loop(BULK_MIDDLE, n_pairs, lambda i: send_bulk(*couple(i)))
    advect(blocks - 1)

    loop(0, 2, lambda i: send_bulk(*single(i)))

    s_last.wait_recv()
    press = baroclinic_rate / levels

    def pressure(i):
        over = s_over[tall(i), :]
        dens = [
            haline_coef * trp[0, l, mid(i, TALL), :] - thermal_coef * trp[1, l, mid(i, TALL), :]
            for l in range(2)
        ]
        d = press * dpp[mid(i, TALL), :]
        pp[0, tall(i), :] = d * (over + 0.5 * dens[0])
        pp[1, tall(i), :] = d * (over + dens[0] + 0.5 * dens[1])

    loop(0, talls, pressure)

    @pl.when(up_there)
    def _():
        x_down.wait_recv()

    @pl.when(down_there)
    def _():
        x_up.wait_recv()

    for copy in flow_copies:
        copy.wait_recv()
    flow_sum = (xt[flows, :] + er[0]) + (er[1] + er[2])
    xr[flows, :] = flow_sum
    yb[...] = jnp.transpose(xr[...])
    mix_up = jnp.where(up_there, mixing_rate, 0.0).astype(f32)
    mix_down = jnp.where(down_there, mixing_rate, 0.0).astype(f32)
    own_up = (1.0 - mixing_rate) - mix_up
    own_down = (1.0 - mixing_rate) - mix_down

    d_last.wait_recv()
    flow_n, flow_s = flow_sum[2:3, :], flow_sum[3:4, :]

    def surface(i):
        row = i * TALL + sub_t
        across = jnp.where(at_edge, unpacked(yb[tall(i), :], n_uv), 0.0)
        across = across + jnp.where(row == rows - 1, flow_n, jnp.where(row == 0, flow_s, 0.0))
        total = d_all[tall(i), :] + across
        ns = sfb[tall(i), :] - eta_rate * wp[mid(i, TALL), :] * total
        out_s[tall(i), :] = ns
        nsp[tall(i), :] = ns
        p0, p1 = pp[0, tall(i), :], pp[1, tall(i), :]
        c2[tall(i), :] = jnp.where(
            lane_t == 0, ns, jnp.where(lane_t == 1, roll(p0, 1), jnp.where(lane_t == 2, roll(p1, 2), 0.0))
        )

    loop(0, talls, surface)
    r2[...] = zero
    r2[pl.ds(0, 1), :] = nsp[pl.ds(0, 1), :]
    for l in range(2):
        r2[pl.ds(1 + l, 1), :] = pp[l, pl.ds(0, 1), :]
    c2t[...] = jnp.transpose(c2[...])

    @pl.when(gt > 0)
    def _():
        p2_west.start()

    @pl.when(gy > 0)
    def _():
        p2_south.start()

    def blend_edges(i):
        x = xb[tall(i), :]
        is_top = lane_t < 2 * nt
        other = jnp.where(is_top, roll(x, -2 * nt), roll(x, 2 * nt))
        bx[tall(i), :] = (
            jnp.where(is_top, own_up, own_down) * x
            + mixing_rate * other
            + jnp.where(is_top, mix_up, mix_down) * yb[tall(i), :]
        )

    loop(0, talls, blend_edges)

    is_top_level = (g == 0).astype(f32)

    def finish(r):
        w = wp[mid(r), :]
        edge = bx[blk(r), :]
        updated = [[], []]
        for n in range(nt):
            a0, a1 = adv[0, r, n], adv[1, r, n]
            e0 = jnp.where(short_edge, unpacked(edge, n), 0.0)
            e1 = jnp.where(short_edge, unpacked(edge, nt + n), 0.0)
            b0 = (own_up * a0 + mixing_rate * a1) + (mix_up * ga[r, n] + e0)
            b1 = (own_down * a1 + mixing_rate * a0) + (mix_down * gb[r, n] + e1)
            for l, b in enumerate((b0, b1)):
                c = trp[n, l, mid(r), :]
                updated[l].append(c + w * (b - c))
        warm = [w * jnp.exp(warming_rate * updated[l][1]) for l in range(2)]
        cell = (r * 8 + sub) * lanes + lane
        top = is_top_level * w
        hits = [jnp.where(cell == rc[i], top, 0.0) for i in range(rc.shape[0])]
        for n in range(nt):
            k = kb[n, 0]
            react = [k * updated[l][0] for l in range(2)]
            for m in range(1, nt):
                k = kb[n, m]
                react = [react[l] + k * updated[l][m] for l in range(2)]
            source = hits[0] * rl[0, n]
            for i in range(1, rc.shape[0]):
                source = source + hits[i] * rl[i, n]
            out_tr[n, 0, blk(r), :] = updated[0][n] + (warm[0] * react[0] + source)
            out_tr[n, 1, blk(r), :] = updated[1][n] + warm[1] * react[1]

    def finish_couple(i):
        await_bulk(*couple(i))
        loop(2 * i + 1, 2 * i + 3, finish)

    def finish_single(i):
        await_bulk(*single(i))
        finish(i * (blocks - 1))

    loop(0, VELOCITIES_AFTER, finish_couple)

    @pl.when(gt < n_tx - 1)
    def _():
        p2_west.wait_recv()

    @pl.when(gy < n_ty - 1)
    def _():
        p2_south.wait_recv()

    t2[...] = jnp.transpose(e2[...])
    nsp[pl.ds(rows, 1), :] = n2[pl.ds(0, 1), :]
    for l in range(2):
        pp[l, pl.ds(rows, 1), :] = n2[pl.ds(1 + l, 1), :]
    friction = jnp.where(g == n_grp - 1, friction_rate, 0.0).astype(f32)

    def velocities(i):
        m = mb[tall(i), :]
        t = t2[tall(i), :]
        w = wp[mid(i, TALL), :]
        open_e = w * jnp.where(at_east, unpacked(m, f_w), roll(w, -1))
        open_n = w * wp[north(i, TALL), :]
        above = pl.ds(i * TALL + 1, TALL)
        ns = nsp[tall(i), :]
        slope_e = jnp.where(at_east, roll(t, -1), roll(ns, -1)) - ns
        slope_n = nsp[above, :] - ns
        for l in range(2):
            p = pp[l, tall(i), :]
            push_e = jnp.where(at_east, roll(t, -2 - l), roll(p, -1)) - p
            push_n = pp[l, above, :] - p
            for ref, out, field, opened, slope, push in (
                (up, out_u, n_uv + l, open_e, slope_e, push_e),
                (vp, out_v, n_uv + 2 + l, open_n, slope_n, push_n),
            ):
                x = ref[l, mid(i, TALL), :]
                beside = unpacked(m, field)
                lap = (
                    (ref[l, north(i, TALL), :] + ref[l, south(i, TALL), :])
                    + (jnp.where(at_east, beside, roll(x, -1)) + jnp.where(at_west, beside, roll(x, 1)))
                    - 4.0 * x
                )
                new = x - gravity_rate * slope - push + viscous_rate * lap
                if l == 1:
                    new = new - friction * x
                out[l, tall(i), :] = opened * new

    loop(0, talls, velocities)
    loop(VELOCITIES_AFTER, n_pairs, finish_couple)
    loop(0, 2, finish_single)

    for copy in [*d_copies, *s_copies, *flow_copies]:
        copy.wait_send()
    for there, copy in halo_sends + [
        (up_there, x_up),
        (down_there, x_down),
        (gt > 0, p2_west),
        (gy > 0, p2_south),
    ]:

        @pl.when(there)
        def _(copy=copy):
            copy.wait_send()

    loop(0, n_pairs, lambda i: await_sent(*couple(i)))
    loop(0, 2, lambda i: await_sent(*single(i)))


def put_kernel(*refs):
    sources, targets, sem = refs[:4], refs[4:8], refs[8]
    puts = [pltpu.make_async_copy(a, b, sem.at[i]) for i, (a, b) in enumerate(zip(sources, targets))]
    for put in puts:
        put.start()
    for put in puts:
        put.wait()


def shards(tracers, east_velocity, north_velocity, surface, depth, wet_mask, river_cells, river_loads, kinetics):
    nt, own, rows, lanes = tracers.shape
    levels = own * lax.axis_size("grp")
    blocks = rows // 8
    tall = rows + 2 * PAD
    tile = pltpu.VMEM((rows, lanes), f32)
    twice = pltpu.VMEM((2, rows, lanes), f32)
    edges = pltpu.VMEM((2, 40, lanes), f32)
    dma = pltpu.SemaphoreType.DMA
    scratch = [
        pltpu.VMEM((nt, 2, tall, lanes), f32),
        pltpu.VMEM((2, tall, lanes), f32),
        pltpu.VMEM((2, tall, lanes), f32),
        tile,
        pltpu.VMEM((tall, lanes), f32),
        pltpu.VMEM((rows, lanes), jnp.int32),
        pltpu.VMEM((tall, lanes), f32),
        pltpu.VMEM((nt, nt, 8, lanes), f32),
        twice,
        pltpu.VMEM((2, tall, lanes), f32),
        twice,
        pltpu.VMEM((2, rows // 2, lanes), f32),
        pltpu.VMEM((2, rows // 2, lanes), f32),
        pltpu.VMEM((rows // 2, lanes), f32),
        pltpu.VMEM((rows // 2, lanes), f32),
        pltpu.VMEM((rows // 2, lanes), f32),
        tile,
        tile,
        edges,
        edges,
        tile,
        tile,
        edges,
        edges,
        tile,
        tile,
        tile,
        tile,
        tile,
        pltpu.VMEM((3, 8, lanes), f32),
        tile,
        tile,
        pltpu.VMEM((2, blocks, nt, 8, lanes), f32),
        pltpu.VMEM((blocks, nt, 8, lanes), f32),
        pltpu.VMEM((blocks, nt, 8, lanes), f32),
        pltpu.VMEM((rows + 8, lanes), f32),
        pltpu.VMEM((2, rows + 8, lanes), f32),
        tile,
        tile,
        tile,
        tile,
        pltpu.VMEM((8, lanes), f32),
        pltpu.VMEM((8, lanes), f32),
        pltpu.SMEM(river_cells.shape, jnp.int32),
        pltpu.SMEM(river_loads.shape, f32),
        pltpu.SMEM((nt, nt), f32),
        dma((10,)),
        dma((4,)),
        dma((4,)),
        dma((6,)),
        dma((6,)),
        dma((3,)),
        dma((3,)),
        dma((2,)),
        dma((2,)),
        dma((2,)),
        dma((2,)),
        dma((2, blocks)),
        dma((2, blocks)),
    ]
    anywhere = pl.BlockSpec(memory_space=pltpu.HBM)
    vmem = pl.BlockSpec(memory_space=pltpu.VMEM)
    outs = (
        jax.ShapeDtypeStruct(tracers.shape, f32),
        jax.ShapeDtypeStruct(east_velocity.shape, f32),
        jax.ShapeDtypeStruct(north_velocity.shape, f32),
        jax.ShapeDtypeStruct(surface.shape, f32),
    )
    fields = [
        pltpu.with_memory_space_constraint(x, pltpu.HBM)
        for x in (
            tracers, east_velocity, north_velocity, surface, depth, wet_mask,
            river_cells, river_loads, kinetics,
        )
    ]
    results = pl.pallas_call(
        functools.partial(step_kernel, levels),
        out_shape=outs,
        in_specs=[anywhere] * 9,
        out_specs=(vmem,) * 4,
        scratch_shapes=scratch,
        compiler_params=pltpu.CompilerParams(
            collective_id=0, has_side_effects=True, vmem_limit_bytes=32 * 1024 * 1024
        ),
        name="estuary_step",
    )(*fields)
    return pl.pallas_call(
        put_kernel,
        out_shape=outs,
        in_specs=[pl.BlockSpec(memory_space=pl.ANY)] * 4,
        out_specs=(pl.BlockSpec(memory_space=pl.ANY),) * 4,
        scratch_shapes=[dma((4,))],
        compiler_params=pltpu.CompilerParams(vmem_limit_bytes=1024 * 1024),
        name="put",
    )(*results)


def solution(mesh):
    return jax.shard_map(
        shards,
        mesh=mesh,
        in_specs=(
            P(None, "grp", "ty", "tx"),
            P("grp", "ty", "tx"),
            P("grp", "ty", "tx"),
            P("ty", "tx"),
            P("ty", "tx"),
            P("ty", "tx"),
            P(("ty", "tx")),
            P(("ty", "tx"), None),
            P(),
        ),
        out_specs=(
            P(None, "grp", "ty", "tx"),
            P("grp", "ty", "tx"),
            P("grp", "ty", "tx"),
            P("ty", "tx"),
        ),
        check_vma=False,
    )
```

```python
import functools

import jax
import jax.numpy as jnp
from jax import lax
from jax.experimental import pallas as pl
from jax.experimental.pallas import tpu as pltpu
from jax.sharding import PartitionSpec as P

f32 = jnp.float32
MESH = pl.DeviceIdType.MESH

eta_rate = 0.25
gravity_rate = 0.25
baroclinic_rate = 0.4
viscous_rate = 0.1
friction_rate = 0.3
advect_rate = 0.3
mixing_rate = 0.2
haline_coef = 0.8
thermal_coef = 0.2
warming_rate = 0.46

PAD = 8
TALL = 32
BULK_FIRST = 3
BULK_MIDDLE = 4
VELOCITIES_AFTER = 7


def step_kernel(
    levels,
    tr_hbm, u_hbm, v_hbm, sf_hbm, dp_hbm, wm_hbm, rc_hbm, rl_hbm, kin_hbm,
    out_tr, out_u, out_v, out_s,
    trp, up, vp, sfb, dpp, wmb, wp, kb,
    fb, gp, sdb, d_in, s_in, d_half, s_half, s_other, d_all, s_over,
    ns_send, ns_recv, q, qt, ew_send, ew_recv, mt, mb,
    xb, xt, xr, er, yb, bx, adv, ga, gb,
    nsp, pp, c2, c2t, e2, t2, r2, n2,
    rc, rl, kin, load_sem, halo_ss, halo_rs, red_ss, red_rs, e_ss, e_rs, x_ss, x_rs, p2_ss, p2_rs, bulk_ss, bulk_rs,
):
    g, gy, gt = lax.axis_index("grp"), lax.axis_index("ty"), lax.axis_index("tx")
    n_grp, n_ty, n_tx = lax.axis_size("grp"), lax.axis_size("ty"), lax.axis_size("tx")
    nt = tr_hbm.shape[0]
    rows, lanes = sfb.shape
    blocks = rows // 8
    n_uv = 2 * nt
    f_d, f_w = n_uv + 4, n_uv + 5

    up_there, down_there = g > 0, g < n_grp - 1
    first = g + 1 - 2 * lax.rem(g, 2)
    second = n_grp - 1 - g
    third = lax.rem(g + n_grp // 2, n_grp)

    lane = lax.broadcasted_iota(jnp.int32, (8, lanes), 1)
    sub = lax.broadcasted_iota(jnp.int32, (8, lanes), 0)
    short_edge = jnp.logical_or(lane == lanes - 1, lane == 0)
    lane_t = lax.broadcasted_iota(jnp.int32, (TALL, lanes), 1)
    sub_t = lax.broadcasted_iota(jnp.int32, (TALL, lanes), 0)
    pair = lane_t // 2
    even = lax.rem(lane_t, 2) == 0
    at_east, at_west = lane_t == lanes - 1, lane_t == 0
    at_edge = jnp.logical_or(at_east, at_west)

    def roll(x, shift):
        shift = shift % lanes
        return x if shift == 0 else pltpu.roll(x, shift, 1)

    def unpacked(tile, field):
        return roll(tile, lanes - 1 - 2 * field)

    def blk(r):
        return pl.ds(pl.multiple_of(r * 8, 8), 8)

    def part(which, i):
        return pl.ds(pl.multiple_of(which * (rows // 2) + i * TALL, TALL), TALL)

    def tall(i):
        return pl.ds(pl.multiple_of(i * TALL, TALL), TALL)

    def mid(r, n=8):
        return pl.ds(pl.multiple_of(r * n + PAD, 8), n)

    def south(r, n=8):
        return pl.ds(r * n + (PAD - 1), n)

    def north(r, n=8):
        return pl.ds(r * n + (PAD + 1), n)

    neighbours = [
        (gt > 0, {"tx": gt - 1}),
        (gt < n_tx - 1, {"tx": gt + 1}),
        (None, {"grp": first}),
        (None, {"grp": second}),
        (None, {"grp": third}),
        (gy > 0, {"ty": gy - 1}),
        (gy < n_ty - 1, {"ty": gy + 1}),
    ]
    barrier = pltpu.get_barrier_semaphore()
    for there, device in neighbours:
        if there is None:
            pl.semaphore_signal(barrier, inc=1, device_id=device, device_id_type=MESH)
        else:

            @pl.when(there)
            def _(device=device):
                pl.semaphore_signal(barrier, inc=1, device_id=device, device_id_type=MESH)

    inner = pl.ds(PAD, rows)
    loads = [
        pltpu.make_async_copy(u_hbm, up.at[:, inner, :], load_sem.at[0]),
        pltpu.make_async_copy(v_hbm, vp.at[:, inner, :], load_sem.at[1]),
        pltpu.make_async_copy(dp_hbm, dpp.at[inner, :], load_sem.at[2]),
        pltpu.make_async_copy(wm_hbm, wmb, load_sem.at[3]),
        pltpu.make_async_copy(
            tr_hbm.at[pl.ds(0, 2)], trp.at[pl.ds(0, 2), :, inner, :], load_sem.at[4]
        ),
        pltpu.make_async_copy(
            tr_hbm.at[pl.ds(2, nt - 2)], trp.at[pl.ds(2, nt - 2), :, inner, :], load_sem.at[9]
        ),
        pltpu.make_async_copy(sf_hbm, sfb, load_sem.at[5]),
        pltpu.make_async_copy(kin_hbm, kin, load_sem.at[6]),
        pltpu.make_async_copy(rc_hbm, rc, load_sem.at[7]),
        pltpu.make_async_copy(rl_hbm, rl, load_sem.at[8]),
    ]
    for load in loads:
        load.start()

    def remote(src, dst, ss, rs, device):
        return pltpu.make_async_remote_copy(
            src_ref=src, dst_ref=dst, send_sem=ss, recv_sem=rs, device_id=device, device_id_type=MESH
        )

    to_north = remote(ns_send.at[0], ns_recv.at[0], halo_ss.at[0], halo_rs.at[0], {"ty": gy + 1})
    to_south = remote(ns_send.at[1], ns_recv.at[1], halo_ss.at[1], halo_rs.at[1], {"ty": gy - 1})
    to_east = remote(ew_send.at[0], ew_recv.at[0], halo_ss.at[2], halo_rs.at[2], {"tx": gt + 1})
    to_west = remote(ew_send.at[1], ew_recv.at[1], halo_ss.at[3], halo_rs.at[3], {"tx": gt - 1})
    halo_sends = [
        (gy < n_ty - 1, to_north),
        (gy > 0, to_south),
        (gt < n_tx - 1, to_east),
        (gt > 0, to_west),
    ]
    halo_recvs = [
        (gy > 0, to_north),
        (gy < n_ty - 1, to_south),
        (gt > 0, to_east),
        (gt < n_tx - 1, to_west),
    ]
    half = rows // 2
    d_half_at, s_half_at = lax.rem((g + 1) // 2, 2), g // 2

    def half_at(i):
        return pl.ds(pl.multiple_of(i * half, half), half)

    d_mine, d_other = half_at(d_half_at), half_at(1 - d_half_at)
    s_mine, s_theirs = half_at(s_half_at), half_at(1 - s_half_at)

    def reduction(i, src, dst, device):
        return remote(src, dst, red_ss.at[i], red_rs.at[i], {"grp": device})

    d_copies = [
        reduction(0, sdb.at[1, d_other, :], d_in.at[0], first),
        reduction(1, d_half, d_in.at[1], second),
        reduction(2, d_all.at[d_mine, :], d_all.at[d_mine, :], first),
    ]
    s_copies = [
        reduction(3, sdb.at[0, s_theirs, :], s_in.at[0], second),
        reduction(4, s_half, s_in.at[1], first),
        reduction(5, s_other, s_over.at[s_mine, :], second),
    ]
    d_last = reduction(2, d_all.at[d_other, :], d_all.at[d_other, :], first)
    s_last = reduction(5, s_other, s_over.at[s_theirs, :], second)
    flows = pl.ds(4 * nt, 8)
    flow_copies = [
        remote(xt.at[flows, :], er.at[i], e_ss.at[i], e_rs.at[i], {"grp": device})
        for i, device in enumerate((first, second, third))
    ]
    low, high = pl.ds(0, 2 * nt), pl.ds(2 * nt, 2 * nt)
    x_up = remote(xt.at[low, :], xr.at[high, :], x_ss.at[0], x_rs.at[0], {"grp": g - 1})
    x_down = remote(xt.at[high, :], xr.at[low, :], x_ss.at[1], x_rs.at[1], {"grp": g + 1})
    p2_west = remote(
        c2t.at[pl.ds(0, 8), :], e2.at[pl.ds(0, 8), :], p2_ss.at[0], p2_rs.at[0], {"tx": gt - 1}
    )
    p2_south = remote(r2, n2, p2_ss.at[1], p2_rs.at[1], {"ty": gy - 1})

    n_pairs = blocks // 2 - 1

    def blocks_of(i):
        return pl.ds(2 * i + 1, 2)

    def bulk_up(span, sem):
        return remote(adv.at[0, span], gb.at[span], bulk_ss.at[0, sem], bulk_rs.at[0, sem], {"grp": g - 1})

    def bulk_down(span, sem):
        return remote(adv.at[1, span], ga.at[span], bulk_ss.at[1, sem], bulk_rs.at[1, sem], {"grp": g + 1})

    def send_bulk(span, sem):
        @pl.when(up_there)
        def _():
            bulk_up(span, sem).start()

        @pl.when(down_there)
        def _():
            bulk_down(span, sem).start()

    def await_bulk(span, sem):
        @pl.when(up_there)
        def _():
            bulk_down(span, sem).wait_recv()

        @pl.when(down_there)
        def _():
            bulk_up(span, sem).wait_recv()

    def await_sent(span, sem):
        @pl.when(up_there)
        def _():
            bulk_up(span, sem).wait_send()

        @pl.when(down_there)
        def _():
            bulk_down(span, sem).wait_send()

    def single(i):
        return pl.ds(i * (blocks - 1), 1), n_pairs + i

    def couple(i):
        return blocks_of(i), i

    def loop(start, stop, body):
        lax.fori_loop(start, stop, lambda i, c: (body(i), c)[1], 0)

    zero = jnp.zeros((8, lanes), f32)
    zero_t = jnp.zeros((TALL, lanes), f32)
    talls = rows // TALL

    def clear(ref):
        def one(i):
            ref[blk(i), :] = zero

        loop(0, ref.shape[0] // 8, one)

    def clear_ghost(ref):
        def one(i):
            for n in range(nt):
                ref[i, n] = zero

        loop(0, blocks, one)

    @pl.when(jnp.logical_not(up_there))
    def _():
        clear_ghost(ga)
        clear(xr.at[low, :])

    @pl.when(jnp.logical_not(down_there))
    def _():
        clear_ghost(gb)
        clear(xr.at[high, :])

    clear(xr.at[pl.ds(4 * nt + 8, lanes - 4 * nt - 8), :])
    clear(mt.at[pl.ds(80, lanes - 80), :])
    clear(e2.at[pl.ds(8, lanes - 8), :])

    for slot, (there, _) in enumerate(halo_recvs):

        @pl.when(jnp.logical_not(there))
        def _(slot=slot):
            clear(ns_recv.at[slot] if slot < 2 else ew_recv.at[slot - 2])

    @pl.when(gt == n_tx - 1)
    def _():
        e2[pl.ds(0, 8), :] = zero

    @pl.when(gy == n_ty - 1)
    def _():
        n2[...] = zero

    for load in loads[:4]:
        load.wait()
    for edge in (0, PAD + rows):
        dpp[pl.ds(edge, 8), :] = zero
        wp[pl.ds(edge, 8), :] = zero
    for l in range(2):
        gp[l, pl.ds(0, 8), :] = zero

    def wetness(i):
        wp[mid(i, TALL), :] = wmb[tall(i), :].astype(f32)

    loop(0, talls, wetness)

    def north_face(i, n):
        d, w = dpp[mid(i, n), :], wp[mid(i, n), :]
        depth_n = (0.5 / levels) * (d + dpp[north(i, n), :]) * (w * wp[north(i, n), :])
        for l in range(2):
            gp[l, mid(i, n), :] = vp[l, mid(i, n), :] * depth_n

    def faces(i):
        d, w = dpp[mid(i, TALL), :], wp[mid(i, TALL), :]
        depth_e = (0.5 / levels) * (d + roll(d, -1)) * (w * roll(w, -1))
        depth_e = jnp.where(at_east, 0.0, depth_e)
        for l in range(2):
            fb[l, tall(i), :] = up[l, mid(i, TALL), :] * depth_e
        north_face(i, TALL)

    loop(0, talls, faces)

    def divergence(i):
        east = fb[0, tall(i), :] + fb[1, tall(i), :]
        in_n = gp[0, mid(i, TALL), :] + gp[1, mid(i, TALL), :]
        in_s = gp[0, south(i, TALL), :] + gp[1, south(i, TALL), :]
        sdb[1, tall(i), :] = (east - roll(east, 1)) + (in_n - in_s)

    loop(0, talls, divergence)
    loads[4].wait()

    def density(i):
        salt = trp[0, 0, mid(i, TALL), :] + trp[0, 1, mid(i, TALL), :]
        heat = trp[1, 0, mid(i, TALL), :] + trp[1, 1, mid(i, TALL), :]
        sdb[0, tall(i), :] = haline_coef * salt - thermal_coef * heat

    loop(0, talls, density)

    def advect(r):
        d = dpp[mid(r), :]
        scale = (advect_rate * levels) / d
        for l in range(2):
            fe, gn, gs = fb[l, blk(r), :], gp[l, mid(r), :], gp[l, south(r), :]
            fw = roll(fe, 1)
            out = (jnp.maximum(fe, 0.0) - jnp.minimum(fw, 0.0)) + (
                jnp.maximum(gn, 0.0) - jnp.minimum(gs, 0.0)
            )
            own = 1.0 - scale * out
            from_e, from_w = -scale * jnp.minimum(fe, 0.0), scale * jnp.maximum(fw, 0.0)
            from_n, from_s = -scale * jnp.minimum(gn, 0.0), scale * jnp.maximum(gs, 0.0)
            for n in range(nt):
                c = trp[n, l, mid(r), :]
                adv[l, r, n] = (
                    (own * c + from_e * roll(c, -1))
                    + (from_w * roll(c, 1) + from_n * trp[n, l, north(r), :])
                    + from_s * trp[n, l, south(r), :]
                )

    def advect_couple(i):
        advect(2 * i + 1)
        advect(2 * i + 2)

    loads[5].wait()
    loop(0, 1, advect_couple)

    peers = sum(1 if there is None else there.astype(jnp.int32) for there, _ in neighbours)
    pl.semaphore_wait(barrier, peers)
    d_copies[0].start()
    s_copies[0].start()

    send_bulk(*couple(0))
    loop(1, 2, advect_couple)


    def edges(i):
        packed = zero_t
        fields = [trp.at[n, l] for l in range(2) for n in range(nt)]
        fields += [up.at[0], up.at[1], vp.at[0], vp.at[1], dpp, wp]
        for f, field in enumerate(fields):
            packed = jnp.where(pair == f, roll(field[mid(i, TALL), :], 2 * f + 1), packed)
        q[tall(i), :] = packed

    loop(0, talls, edges)
    qt[...] = jnp.transpose(q[...])
    for side in range(2):
        ew_send[side] = qt[pl.ds(side, 40, stride=2), :]

    padded = [trp.at[n, l] for l in range(2) for n in range(nt)]
    padded += [up.at[0], up.at[1], vp.at[0], vp.at[1], dpp, wp]
    for slot in range(2):
        ns_send[slot, pl.ds(32, 8), :] = zero
    for f, ref in enumerate(padded):
        ns_send[0, pl.ds(f, 1), :] = ref[pl.ds(PAD + rows - 1, 1), :]
        ns_send[1, pl.ds(f, 1), :] = ref[pl.ds(PAD, 1), :]

    send_bulk(*couple(1))
    for there, copy in reversed(halo_sends):

        @pl.when(there)
        def _(copy=copy):
            copy.start()

    def advect_and_send(i):
        advect_couple(i)

        @pl.when(jnp.logical_and(i > 2, i <= BULK_FIRST))
        def _():
            send_bulk(*couple(i - 1))

    loop(2, n_pairs, advect_and_send)

    d_copies[0].wait_recv()
    s_copies[0].wait_recv()
    own_to_first = (g < n_grp - 1).astype(f32)
    second_to_first = (g > 0).astype(f32)

    def first_sums(i):
        d_half[tall(i), :] = sdb[1, part(d_half_at, i), :] + d_in[0, tall(i), :]
        s_half[tall(i), :] = (
            own_to_first * sdb[0, part(s_half_at, i), :] + second_to_first * s_in[0, tall(i), :]
        )

    loop(0, half // TALL, first_sums)

    for load in loads[6:]:
        load.wait()

    def spread(n):
        for m in range(nt):
            kb[n, m] = jnp.full((8, lanes), kin[n, m], f32)

    loop(0, nt, spread)
    d_copies[1].start()
    s_copies[1].start()
    loop(BULK_FIRST, BULK_MIDDLE, lambda i: send_bulk(*couple(i)))

    for there, copy in halo_recvs:

        @pl.when(there)
        def _(copy=copy):
            copy.wait_recv()

    for f, ref in enumerate(padded):
        ref[pl.ds(PAD - 1, 1), :] = ns_recv[0, pl.ds(f, 1), :]
        ref[pl.ds(PAD + rows, 1), :] = ns_recv[1, pl.ds(f, 1), :]
    d_south, w_south = dpp[pl.ds(PAD - 1, 1), :], wp[pl.ds(PAD - 1, 1), :]
    d_row, w_row = dpp[pl.ds(PAD, 1), :], wp[pl.ds(PAD, 1), :]
    depth_s = (0.5 / levels) * (d_south + d_row) * (w_south * w_row)
    for l in range(2):
        gp[l, pl.ds(PAD - 1, 1), :] = vp[l, pl.ds(PAD - 1, 1), :] * depth_s
    north_face(blocks - 1, 8)
    for side in range(2):
        mt[pl.ds(side, 40, stride=2), :] = ew_recv[1 - side]
    mb[...] = jnp.transpose(mt[...])

    def rim(i):
        m = mb[tall(i), :]
        d, w = dpp[mid(i, TALL), :], wp[mid(i, TALL), :]
        scale = (advect_rate * levels) / d
        depth_f = (0.5 / levels) * (d + unpacked(m, f_d)) * (w * unpacked(m, f_w))
        total = zero_t
        parts = []
        for l in range(2):
            flow = jnp.where(at_west, unpacked(m, n_uv + l), up[l, mid(i, TALL), :])
            flux = jnp.where(at_edge, flow * depth_f, 0.0)
            total = total + jnp.where(at_east, flux, -flux)
            z = scale * flux
            z_e = jnp.broadcast_to(z[:, lanes - 1 : lanes], (TALL, lanes))
            z_w = jnp.broadcast_to(z[:, 0:1], (TALL, lanes))
            parts.append(jnp.where(even, -z_e, z_w))
        zz = jnp.where(lane_t < 2 * nt, parts[0], parts[1])
        x = jnp.minimum(zz, 0.0) * q[tall(i), :] + jnp.maximum(zz, 0.0) * m
        xb[tall(i), :] = jnp.where(pair == n_uv, roll(total, 2 * n_uv + 1), x)

    loop(0, talls, rim)
    xt[...] = jnp.transpose(xb[...])
    xt[pl.ds(4 * nt + 2, 1), :] = gp[0, pl.ds(PAD + rows - 1, 1), :] + gp[1, pl.ds(PAD + rows - 1, 1), :]
    xt[pl.ds(4 * nt + 3, 1), :] = -(gp[0, pl.ds(PAD - 1, 1), :] + gp[1, pl.ds(PAD - 1, 1), :])
    d_copies[1].wait_recv()
    s_copies[1].wait_recv()
    above_1, above_2 = (g > 0).astype(f32), (g > 1).astype(f32)
    other_1, other_2 = (g < n_grp - 1).astype(f32), (g < 2).astype(f32)

    def second_sums(i):
        d_all[part(d_half_at, i), :] = d_half[tall(i), :] + d_in[1, tall(i), :]
        got = s_in[1, tall(i), :]
        s_over[part(s_half_at, i), :] = above_1 * got + above_2 * s_in[0, tall(i), :]
        s_other[tall(i), :] = other_1 * got + other_2 * sdb[0, part(s_half_at, i), :]

    loop(0, half // TALL, second_sums)
    advect(0)
    for copy in reversed(flow_copies):
        copy.start()
    d_copies[2].start()
    s_copies[2].start()

    @pl.when(up_there)
    def _():
        x_up.start()

    @pl.when(down_there)
    def _():
        x_down.start()

    loop(BULK_MIDDLE, n_pairs, lambda i: send_bulk(*couple(i)))
    advect(blocks - 1)

    loop(0, 2, lambda i: send_bulk(*single(i)))

    s_last.wait_recv()
    press = baroclinic_rate / levels

    def pressure(i):
        over = s_over[tall(i), :]
        dens = [
            haline_coef * trp[0, l, mid(i, TALL), :] - thermal_coef * trp[1, l, mid(i, TALL), :]
            for l in range(2)
        ]
        d = press * dpp[mid(i, TALL), :]
        pp[0, tall(i), :] = d * (over + 0.5 * dens[0])
        pp[1, tall(i), :] = d * (over + dens[0] + 0.5 * dens[1])

    loop(0, talls, pressure)

    @pl.when(up_there)
    def _():
        x_down.wait_recv()

    @pl.when(down_there)
    def _():
        x_up.wait_recv()

    for copy in flow_copies:
        copy.wait_recv()
    flow_sum = (xt[flows, :] + er[0]) + (er[1] + er[2])
    xr[flows, :] = flow_sum
    yb[...] = jnp.transpose(xr[...])
    mix_up = jnp.where(up_there, mixing_rate, 0.0).astype(f32)
    mix_down = jnp.where(down_there, mixing_rate, 0.0).astype(f32)
    own_up = (1.0 - mixing_rate) - mix_up
    own_down = (1.0 - mixing_rate) - mix_down

    d_last.wait_recv()
    flow_n, flow_s = flow_sum[2:3, :], flow_sum[3:4, :]

    def surface(i):
        row = i * TALL + sub_t
        across = jnp.where(at_edge, unpacked(yb[tall(i), :], n_uv), 0.0)
        across = across + jnp.where(row == rows - 1, flow_n, jnp.where(row == 0, flow_s, 0.0))
        total = d_all[tall(i), :] + across
        ns = sfb[tall(i), :] - eta_rate * wp[mid(i, TALL), :] * total
        out_s[tall(i), :] = ns
        nsp[tall(i), :] = ns
        p0, p1 = pp[0, tall(i), :], pp[1, tall(i), :]
        c2[tall(i), :] = jnp.where(
            lane_t == 0, ns, jnp.where(lane_t == 1, roll(p0, 1), jnp.where(lane_t == 2, roll(p1, 2), 0.0))
        )

    loop(0, talls, surface)
    r2[...] = zero
    r2[pl.ds(0, 1), :] = nsp[pl.ds(0, 1), :]
    for l in range(2):
        r2[pl.ds(1 + l, 1), :] = pp[l, pl.ds(0, 1), :]
    c2t[...] = jnp.transpose(c2[...])

    @pl.when(gt > 0)
    def _():
        p2_west.start()

    @pl.when(gy > 0)
    def _():
        p2_south.start()

    def blend_edges(i):
        x = xb[tall(i), :]
        is_top = lane_t < 2 * nt
        other = jnp.where(is_top, roll(x, -2 * nt), roll(x, 2 * nt))
        bx[tall(i), :] = (
            jnp.where(is_top, own_up, own_down) * x
            + mixing_rate * other
            + jnp.where(is_top, mix_up, mix_down) * yb[tall(i), :]
        )

    loop(0, talls, blend_edges)

    is_top_level = (g == 0).astype(f32)

    def finish(r):
        w = wp[mid(r), :]
        edge = bx[blk(r), :]
        updated = [[], []]
        for n in range(nt):
            a0, a1 = adv[0, r, n], adv[1, r, n]
            e0 = jnp.where(short_edge, unpacked(edge, n), 0.0)
            e1 = jnp.where(short_edge, unpacked(edge, nt + n), 0.0)
            b0 = (own_up * a0 + mixing_rate * a1) + (mix_up * ga[r, n] + e0)
            b1 = (own_down * a1 + mixing_rate * a0) + (mix_down * gb[r, n] + e1)
            for l, b in enumerate((b0, b1)):
                c = trp[n, l, mid(r), :]
                updated[l].append(c + w * (b - c))
        warm = [w * jnp.exp(warming_rate * updated[l][1]) for l in range(2)]
        cell = (r * 8 + sub) * lanes + lane
        top = is_top_level * w
        hits = [jnp.where(cell == rc[i], top, 0.0) for i in range(rc.shape[0])]
        for n in range(nt):
            k = kb[n, 0]
            react = [k * updated[l][0] for l in range(2)]
            for m in range(1, nt):
                k = kb[n, m]
                react = [react[l] + k * updated[l][m] for l in range(2)]
            source = hits[0] * rl[0, n]
            for i in range(1, rc.shape[0]):
                source = source + hits[i] * rl[i, n]
            out_tr[n, 0, blk(r), :] = updated[0][n] + (warm[0] * react[0] + source)
            out_tr[n, 1, blk(r), :] = updated[1][n] + warm[1] * react[1]

    def finish_couple(i):
        await_bulk(*couple(i))
        loop(2 * i + 1, 2 * i + 3, finish)

    def finish_single(i):
        await_bulk(*single(i))
        finish(i * (blocks - 1))

    loop(0, VELOCITIES_AFTER, finish_couple)

    @pl.when(gt < n_tx - 1)
    def _():
        p2_west.wait_recv()

    @pl.when(gy < n_ty - 1)
    def _():
        p2_south.wait_recv()

    t2[...] = jnp.transpose(e2[...])
    nsp[pl.ds(rows, 1), :] = n2[pl.ds(0, 1), :]
    for l in range(2):
        pp[l, pl.ds(rows, 1), :] = n2[pl.ds(1 + l, 1), :]
    friction = jnp.where(g == n_grp - 1, friction_rate, 0.0).astype(f32)

    def velocities(i):
        m = mb[tall(i), :]
        t = t2[tall(i), :]
        w = wp[mid(i, TALL), :]
        open_e = w * jnp.where(at_east, unpacked(m, f_w), roll(w, -1))
        open_n = w * wp[north(i, TALL), :]
        above = pl.ds(i * TALL + 1, TALL)
        ns = nsp[tall(i), :]
        slope_e = jnp.where(at_east, roll(t, -1), roll(ns, -1)) - ns
        slope_n = nsp[above, :] - ns
        for l in range(2):
            p = pp[l, tall(i), :]
            push_e = jnp.where(at_east, roll(t, -2 - l), roll(p, -1)) - p
            push_n = pp[l, above, :] - p
            for ref, out, field, opened, slope, push in (
                (up, out_u, n_uv + l, open_e, slope_e, push_e),
                (vp, out_v, n_uv + 2 + l, open_n, slope_n, push_n),
            ):
                x = ref[l, mid(i, TALL), :]
                beside = unpacked(m, field)
                lap = (
                    (ref[l, north(i, TALL), :] + ref[l, south(i, TALL), :])
                    + (jnp.where(at_east, beside, roll(x, -1)) + jnp.where(at_west, beside, roll(x, 1)))
                    - 4.0 * x
                )
                new = x - gravity_rate * slope - push + viscous_rate * lap
                if l == 1:
                    new = new - friction * x
                out[l, tall(i), :] = opened * new

    loop(0, talls, velocities)
    loop(VELOCITIES_AFTER, n_pairs, finish_couple)
    loop(0, 2, finish_single)

    for copy in [*d_copies, *s_copies, *flow_copies]:
        copy.wait_send()
    for there, copy in halo_sends + [
        (up_there, x_up),
        (down_there, x_down),
        (gt > 0, p2_west),
        (gy > 0, p2_south),
    ]:

        @pl.when(there)
        def _(copy=copy):
            copy.wait_send()

    loop(0, n_pairs, lambda i: await_sent(*couple(i)))
    loop(0, 2, lambda i: await_sent(*single(i)))


def put_kernel(*refs):
    sources, targets, sem = refs[:4], refs[4:8], refs[8]
    puts = [pltpu.make_async_copy(a, b, sem.at[i]) for i, (a, b) in enumerate(zip(sources, targets))]
    for put in puts:
        put.start()
    for put in puts:
        put.wait()


def shards(tracers, east_velocity, north_velocity, surface, depth, wet_mask, river_cells, river_loads, kinetics):
    nt, own, rows, lanes = tracers.shape
    levels = own * lax.axis_size("grp")
    blocks = rows // 8
    tall = rows + 2 * PAD
    tile = pltpu.VMEM((rows, lanes), f32)
    twice = pltpu.VMEM((2, rows, lanes), f32)
    edges = pltpu.VMEM((2, 40, lanes), f32)
    dma = pltpu.SemaphoreType.DMA
    scratch = [
        pltpu.VMEM((nt, 2, tall, lanes), f32),
        pltpu.VMEM((2, tall, lanes), f32),
        pltpu.VMEM((2, tall, lanes), f32),
        tile,
        pltpu.VMEM((tall, lanes), f32),
        pltpu.VMEM((rows, lanes), jnp.int32),
        pltpu.VMEM((tall, lanes), f32),
        pltpu.VMEM((nt, nt, 8, lanes), f32),
        twice,
        pltpu.VMEM((2, tall, lanes), f32),
        twice,
        pltpu.VMEM((2, rows // 2, lanes), f32),
        pltpu.VMEM((2, rows // 2, lanes), f32),
        pltpu.VMEM((rows // 2, lanes), f32),
        pltpu.VMEM((rows // 2, lanes), f32),
        pltpu.VMEM((rows // 2, lanes), f32),
        tile,
        tile,
        edges,
        edges,
        tile,
        tile,
        edges,
        edges,
        tile,
        tile,
        tile,
        tile,
        tile,
        pltpu.VMEM((3, 8, lanes), f32),
        tile,
        tile,
        pltpu.VMEM((2, blocks, nt, 8, lanes), f32),
        pltpu.VMEM((blocks, nt, 8, lanes), f32),
        pltpu.VMEM((blocks, nt, 8, lanes), f32),
        pltpu.VMEM((rows + 8, lanes), f32),
        pltpu.VMEM((2, rows + 8, lanes), f32),
        tile,
        tile,
        tile,
        tile,
        pltpu.VMEM((8, lanes), f32),
        pltpu.VMEM((8, lanes), f32),
        pltpu.SMEM(river_cells.shape, jnp.int32),
        pltpu.SMEM(river_loads.shape, f32),
        pltpu.SMEM((nt, nt), f32),
        dma((10,)),
        dma((4,)),
        dma((4,)),
        dma((6,)),
        dma((6,)),
        dma((3,)),
        dma((3,)),
        dma((2,)),
        dma((2,)),
        dma((2,)),
        dma((2,)),
        dma((2, blocks)),
        dma((2, blocks)),
    ]
    anywhere = pl.BlockSpec(memory_space=pltpu.HBM)
    vmem = pl.BlockSpec(memory_space=pltpu.VMEM)
    outs = (
        jax.ShapeDtypeStruct(tracers.shape, f32),
        jax.ShapeDtypeStruct(east_velocity.shape, f32),
        jax.ShapeDtypeStruct(north_velocity.shape, f32),
        jax.ShapeDtypeStruct(surface.shape, f32),
    )
    fields = [
        pltpu.with_memory_space_constraint(x, pltpu.HBM)
        for x in (
            tracers, east_velocity, north_velocity, surface, depth, wet_mask,
            river_cells, river_loads, kinetics,
        )
    ]
    results = pl.pallas_call(
        functools.partial(step_kernel, levels),
        out_shape=outs,
        in_specs=[anywhere] * 9,
        out_specs=(vmem,) * 4,
        scratch_shapes=scratch,
        compiler_params=pltpu.CompilerParams(
            collective_id=0, has_side_effects=True, vmem_limit_bytes=32 * 1024 * 1024
        ),
        name="estuary_step",
    )(*fields)
    return pl.pallas_call(
        put_kernel,
        out_shape=outs,
        in_specs=[pl.BlockSpec(memory_space=pl.ANY)] * 4,
        out_specs=(pl.BlockSpec(memory_space=pl.ANY),) * 4,
        scratch_shapes=[dma((4,))],
        compiler_params=pltpu.CompilerParams(vmem_limit_bytes=1024 * 1024),
        name="put",
    )(*results)


def solution(mesh):
    return jax.shard_map(
        shards,
        mesh=mesh,
        in_specs=(
            P(None, "grp", "ty", "tx"),
            P("grp", "ty", "tx"),
            P("grp", "ty", "tx"),
            P("ty", "tx"),
            P("ty", "tx"),
            P("ty", "tx"),
            P(("ty", "tx")),
            P(("ty", "tx"), None),
            P(),
        ),
        out_specs=(
            P(None, "grp", "ty", "tx"),
            P("grp", "ty", "tx"),
            P("grp", "ty", "tx"),
            P("ty", "tx"),
        ),
        check_vma=False,
    )
```
